32 devices in a mesh: batch: 2 (over x), row: 4 (over z), col: 4 (over y, core).
Axes of the slice: x: 2, y: 2, z: 4, core: 2. Of those that a mesh axis runs over, the one named last changes fastest.
Arguments:
- spd_blocks: float32 [64, 256, 8192], P(('batch', 'row'), None, 'col'), parts along dimension 0
Outputs:
- output: float32 [64, 256, 8192], P(('batch', 'row'), None, 'col'), parts along dimension 0
There are 2 independent parts. The reference program is written for one: setup_inputs(seed, part) draws one part's arguments, and reference() takes and returns one part's arrays. A program takes and returns all parts, laid end to end along the dimension named above; each array names one.
All inputs are finite; a program needn't handle non-finite values.
Results may differ from the reference program's by a relative error of at most 0.001.
Values are sent between devices in bfloat16 or wider.
A program may use at most 1 GiB of HBM per device.

```python
import math
import jax
import jax.numpy as jnp
from jax import lax

BLOCK = 256
ORDER = 8192
ROW_DEVS = 4
COL_DEVS = 4

BLOCK_COUNT = ORDER // BLOCK


def to_logical(a_cyc):
    by_rows = a_cyc.reshape(ROW_DEVS, BLOCK_COUNT // ROW_DEVS, BLOCK, ORDER).transpose(1, 0, 2, 3)
    by_cols = by_rows.reshape(ORDER, COL_DEVS, BLOCK_COUNT // COL_DEVS, BLOCK).transpose(0, 2, 1, 3)
    return by_cols.reshape(ORDER, ORDER)


def to_cyclic(matrix):
    by_rows = matrix.reshape(BLOCK_COUNT // ROW_DEVS, ROW_DEVS, BLOCK, ORDER).transpose(1, 0, 2, 3)
    by_cols = by_rows.reshape(ORDER, BLOCK_COUNT // COL_DEVS, COL_DEVS, BLOCK).transpose(0, 2, 1, 3)
    return by_cols.reshape(BLOCK_COUNT, BLOCK, ORDER)


def setup_inputs(seed: int = 0, part: int = 0) -> dict:
    rng_key = jax.random.fold_in(jax.random.key(seed), part)
    gauss_draw = jax.random.normal(rng_key, (ORDER, ORDER), jnp.float32)
    sym_part = (gauss_draw + gauss_draw.T) * math.sqrt(0.5 / ORDER)
    matrix = (sym_part + 2.2 * jnp.eye(ORDER, dtype=jnp.float32)) * ORDER
    return {"spd_blocks": to_cyclic(matrix)}


def reference(spd_blocks):
    trailing = to_logical(spd_blocks)
    columns = []
    for step_idx in range(BLOCK_COUNT):
        diag_fac = jnp.tril(jnp.linalg.cholesky(trailing[:BLOCK, :BLOCK]))
        pieces = [jnp.zeros((step_idx * BLOCK, BLOCK), jnp.float32), diag_fac]
        if step_idx + 1 < BLOCK_COUNT:
            panel_f32 = lax.linalg.triangular_solve(diag_fac, trailing[BLOCK:, :BLOCK], left_side=False, lower=True, transpose_a=True)
            pieces.append(panel_f32)
            panel_b16 = panel_f32.astype(jnp.bfloat16)
            trailing = trailing[BLOCK:, BLOCK:] - jnp.dot(panel_b16, panel_b16.T, preferred_element_type=jnp.float32)
        columns.append(jnp.concatenate(pieces, axis=0))
    return to_cyclic(jnp.concatenate(columns, axis=1))
```

```python
import functools

import jax
import jax.numpy as jnp
from jax import lax
from jax.experimental import pallas as pl
from jax.experimental.pallas import tpu as pltpu
from jax.sharding import PartitionSpec as P

MESH = pl.DeviceIdType.MESH
HIGH = lax.Precision.HIGHEST
GRID = 4
BLK = 256
HALF = 128
PAN = 16
SLOTS = 4
F32, B16 = jnp.float32, jnp.bfloat16
NT = (((1,), (1,)), ((), ()))
TN = (((0,), (0,)), ((), ()))


def split3(x):
    hi = x.astype(B16)
    rest = x - hi.astype(F32)
    mid = rest.astype(B16)
    return hi, mid, (rest - mid.astype(F32)).astype(B16)


def gram(left, right):
    a1, a2, a3 = split3(left)
    b1, b2, b3 = split3(right)
    lhs = jnp.concatenate([a1, a1, a2, a2, a1, a3], axis=0)
    rhs = jnp.concatenate([b1, b2, b1, b2, b3, b1], axis=0)
    return lax.dot_general(lhs, rhs, TN, preferred_element_type=F32)


def eliminate(rows, base):
    groups = rows.shape[0]
    cols = [jnp.broadcast_to(rows[0][:, base + t : base + t + 1], (PAN, HALF))[None] for t in range(PAN)]
    work = jnp.concatenate(cols + [rows], axis=0)
    sub = lax.broadcasted_iota(jnp.int32, (PAN, HALF), 0)
    scale = jnp.zeros((PAN, HALF), F32)
    for t in range(PAN):
        root = jnp.broadcast_to(lax.rsqrt(work[0, t : t + 1, :]), (PAN, HALF))
        scale = jnp.where(sub == t, root, scale)
        mult = jnp.where(sub > t, work[0] * (root * root), 0.0)
        work = work[1:]
        work = work - mult[None] * work[:, t : t + 1, :]
    return work[-groups:] * scale[None]


def factor_half(tab):
    count = HALF // PAN
    groups = tab.shape[1] // HALF
    done = []
    for p in range(count):
        own = tab[:PAN]
        rows = jnp.concatenate([own[None, :, g * HALF : (g + 1) * HALF] for g in range(groups)], axis=0)
        out = eliminate(rows, p * PAN)
        flat = jnp.concatenate([out[g] for g in range(groups)], axis=1)
        done.append(flat)
        if p + 1 < count:
            tab = tab[PAN:] - gram(flat[:, :HALF], flat)[(p + 1) * PAN :]
    return jnp.concatenate(done, axis=0)


def kernel(nb, a_ref, o_ref, mat, row_pan, col_pan, inv_a, inv_b, load_sem, br_recv, bc_recv, row_send, chain_send,
           inv_recv, inv_send, row_free, inv_free, chain_free):
    r = lax.axis_index("row")
    c = lax.axis_index("col")
    steps = nb * GRID
    last = GRID * (nb - 1)

    def first_block(k, pos):
        return lax.div(k + GRID - pos, GRID)

    def rows_of(t):
        return pl.ds(pl.multiple_of(t * BLK, BLK), BLK)

    def load(t, s):
        return pltpu.make_async_copy(a_ref.at[t, :, pl.ds(s * BLK, BLK)], mat.at[s, pl.ds(t * BLK, BLK), :], load_sem.at[t, s])

    def store(t, s):
        return pltpu.make_async_copy(mat.at[s, pl.ds(t * BLK, BLK), :], o_ref.at[t, :, pl.ds(s * BLK, BLK)], load_sem.at[t, s])

    for s in range(nb):
        for t in range(nb):
            load(t, s).start()

    barrier = pltpu.get_barrier_semaphore()
    for off in range(1, GRID):
        pl.semaphore_signal(barrier, inc=1, device_id={"row": lax.rem(r + off, GRID)}, device_id_type=MESH)
        pl.semaphore_signal(barrier, inc=1, device_id={"col": lax.rem(c + off, GRID)}, device_id_type=MESH)
    pl.semaphore_wait(barrier, 2 * (GRID - 1))

    for s in range(nb):
        for t in range(nb):
            load(t, s).wait()

    def row_copy(slot, t, off):
        return pltpu.make_async_remote_copy(
            src_ref=row_pan.at[slot, rows_of(t), :], dst_ref=row_pan.at[slot, rows_of(t), :],
            send_sem=row_send.at[off - 1, t], recv_sem=br_recv.at[slot, t],
            device_id={"col": lax.rem(c + off, GRID)}, device_id_type=MESH)

    def chain_copy(src, slot, s, way):
        return pltpu.make_async_remote_copy(
            src_ref=src.at[slot, rows_of(s), :], dst_ref=col_pan.at[slot, rows_of(s), :],
            send_sem=chain_send.at[slot, way, s], recv_sem=bc_recv.at[slot, s],
            device_id={"row": r + 1 - 2 * way}, device_id_type=MESH)

    def inv_copy(off, part):
        ref = (inv_a, inv_b)[part]
        return pltpu.make_async_remote_copy(
            src_ref=ref, dst_ref=ref, send_sem=inv_send.at[off - 1, part], recv_sem=inv_recv.at[part],
            device_id={"row": lax.rem(r + off, GRID)}, device_id_type=MESH)

    def sends(way):
        return ((r >= c) & (r < GRID - 1)) if way == 0 else ((r <= c) & (r > 0))

    def pass_on(src, k, s):
        slot = lax.rem(k, SLOTS)
        for way in range(2):
            @pl.when(sends(way))
            def _():
                @pl.when((s == first_block(k, c)) & (k >= SLOTS))
                def _():
                    pl.semaphore_wait(chain_free.at[way], 1)
                chain_copy(src, slot, s, way).start()

    def own_col_block(k, s):
        slot = lax.rem(k, SLOTS)
        col_pan[slot, rows_of(s), :] = row_pan[slot, rows_of(s), :]
        pass_on(row_pan, k, s)

    def take_row(k, t):
        row_copy(lax.rem(k, SLOTS), t, 1).wait_recv()

        @pl.when(r == c)
        def _():
            own_col_block(k, t)

    def take_col(k, s):
        chain_copy(col_pan, lax.rem(k, SLOTS), s, 0).wait_recv()
        pass_on(col_pan, k, s)

    def update(k, t, s, count):
        slot = lax.rem(k, SLOTS)
        span = pl.ds(pl.multiple_of(t * BLK, BLK), count * BLK)
        prod = lax.dot_general(row_pan[slot, span, :], col_pan[slot, rows_of(s), :], NT, preferred_element_type=F32)
        mat[s, span, :] = mat[s, span, :] - prod

    def loop(lo, hi, body):
        def run(i, carry):
            body(i)
            return carry
        lax.fori_loop(lo, hi, run, 0)

    def factor_diag(k):
        t0 = lax.div(k, GRID)
        blk = mat[t0, rows_of(t0), :]
        eye = (lax.broadcasted_iota(jnp.int32, (HALF, HALF), 0) == lax.broadcasted_iota(jnp.int32, (HALF, HALF), 1)).astype(F32)

        def for_peers(act):
            for off in range(1, GRID):
                @pl.when(k < last + lax.rem(r + off, GRID))
                def _():
                    act(off)

        @pl.when(k >= GRID)
        def _():
            for_peers(lambda off: pl.semaphore_wait(inv_free.at[off - 1], 1))

        top = factor_half(jnp.concatenate([blk[:HALF], eye], axis=1))
        inv_a[...] = top[:, 2 * HALF :]
        for_peers(lambda off: inv_copy(off, 0).start())
        mid = lax.dot_general(top[:, HALF : 2 * HALF], top[:, HALF:], TN, precision=HIGH, preferred_element_type=F32)
        low = factor_half(jnp.concatenate([blk[HALF:, HALF:] - mid[:, :HALF], -mid[:, HALF:], eye], axis=1))
        inv_b[...] = low[:, HALF:]
        for_peers(lambda off: inv_copy(off, 1).start())
        zero = jnp.zeros((HALF, HALF), F32)
        up = lax.broadcasted_iota(jnp.int32, (HALF, HALF), 0) <= lax.broadcasted_iota(jnp.int32, (HALF, HALF), 1)
        left = jnp.concatenate([jnp.where(up, top[:, :HALF], 0.0).T, top[:, HALF : 2 * HALF].T], axis=0)
        right = jnp.concatenate([zero, jnp.where(up, low[:, :HALF], 0.0).T], axis=0)
        mat[t0, rows_of(t0), :] = jnp.concatenate([left, right], axis=1)

    def solve_col(k):
        t0 = lax.div(k, GRID)
        slot = lax.rem(k, SLOTS)

        @pl.when(k < last + r)
        def _():
            @pl.when(r != c)
            def _():
                inv_copy(1, 0).wait_recv()
                inv_copy(1, 1).wait_recv()

            @pl.when(k >= SLOTS)
            def _():
                pl.semaphore_wait(row_free, GRID - 1)

        def one(t):
            inv = jnp.concatenate(
                [jnp.concatenate([inv_a[...], jnp.zeros((HALF, HALF), F32)], axis=1), inv_b[...]], axis=0)
            sol = lax.dot_general(mat[t0, rows_of(t), :], inv, NT, precision=HIGH, preferred_element_type=F32)
            mat[t0, rows_of(t), :] = sol
            row_pan[slot, rows_of(t), :] = sol.astype(B16)
            for off in range(1, GRID):
                row_copy(slot, t, off).start()

            @pl.when(r == c)
            def _():
                own_col_block(k, t)

        loop(first_block(k, r), nb, one)

        @pl.when(r == c)
        def _():
            for off in range(1, GRID):
                @pl.when(k < last + lax.rem(r + off, GRID))
                def _():
                    inv_copy(off, 0).wait_send()
                    inv_copy(off, 1).wait_send()

        @pl.when((r != c) & (k + GRID < last + r))
        def _():
            pl.semaphore_signal(inv_free.at[lax.rem(r - c + GRID, GRID) - 1], inc=1, device_id={"row": lax.rem(k, GRID)}, device_id_type=MESH)

    def trail(k):
        d = lax.rem(k, GRID)
        nxt = lax.rem(k + 1, GRID)
        t_lo = first_block(k, r)
        s_lo = first_block(k, c) + jnp.where(c == nxt, 1, 0)

        @pl.when((c != d) & (c != nxt))
        def _():
            loop(t_lo, nb, lambda t: take_row(k, t))

        @pl.when(r != c)
        def _():
            loop(s_lo, nb, lambda s: take_col(k, s))

        def column(s):
            lo = jnp.maximum(t_lo, s)
            pairs = lax.div(nb - lo, 2)
            loop(0, pairs, lambda q: update(k, lo + 2 * q, s, 2))

            @pl.when(lax.rem(nb - lo, 2) == 1)
            def _():
                update(k, nb - 1, s, 1)

        loop(s_lo, nb, column)

    def finish(k):
        d = lax.rem(k, GRID)

        @pl.when(c == d)
        def _():
            def one(t):
                for off in range(1, GRID):
                    row_copy(lax.rem(k, SLOTS), t, off).wait_send()
            loop(first_block(k, r), nb, one)

        for way in range(2):
            @pl.when(sends(way))
            def _():
                loop(first_block(k, c), nb, lambda s: chain_copy(col_pan, lax.rem(k, SLOTS), s, way).wait_send())

        @pl.when((c != d) & (k + SLOTS < last + r))
        def _():
            pl.semaphore_signal(row_free, inc=1, device_id={"col": d}, device_id_type=MESH)

        for way in range(2):
            @pl.when((k + SLOTS < last + c) & ((r > c) if way == 0 else (r < c)))
            def _():
                pl.semaphore_signal(chain_free.at[way], inc=1, device_id={"row": r - 1 + 2 * way}, device_id_type=MESH)

    def ahead(k):
        s1 = lax.div(k + 1, GRID)

        @pl.when(r == c)
        def _():
            take_row(k, s1)
            update(k, s1, s1, 1)

        @pl.when(r != c)
        def _():
            take_col(k, s1)

            def one(t):
                take_row(k, t)
                update(k, t, s1, 1)
            loop(first_block(k, r), nb, one)

    def ahead_rest(k):
        s1 = lax.div(k + 1, GRID)

        def one(t):
            take_row(k, t)
            update(k, t, s1, 1)
        loop(s1 + 1, nb, one)

    def step(k):
        d = lax.rem(k, GRID)

        @pl.when(c == d)
        def _():
            @pl.when(r == d)
            def _():
                factor_diag(k)

                @pl.when(k > 0)
                def _():
                    ahead_rest(k - 1)
            solve_col(k)

        @pl.when(k > 0)
        def _():
            trail(k - 1)

        @pl.when(k > 1)
        def _():
            finish(k - 2)

        @pl.when((c == lax.rem(k + 1, GRID)) & (k + 1 < steps))
        def _():
            ahead(k)

    loop(0, steps, step)
    finish(steps - 2)

    for s in range(nb):
        for t in range(nb):
            store(t, s).start()
    for s in range(nb):
        for t in range(nb):
            store(t, s).wait()


def solution(mesh):
    def factor_local(a_loc):
        nb, blk, width = a_loc.shape
        dma = pltpu.SemaphoreType.DMA
        reg = pltpu.SemaphoreType.REGULAR
        work = pl.pallas_call(
            functools.partial(kernel, nb),
            out_shape=jax.ShapeDtypeStruct(a_loc.shape, F32),
            in_specs=[pl.BlockSpec(memory_space=pl.ANY)],
            out_specs=pl.BlockSpec(memory_space=pl.ANY),
            scratch_shapes=[
                pltpu.VMEM((nb, nb * blk, blk), F32),
                pltpu.VMEM((SLOTS, nb * blk, blk), B16),
                pltpu.VMEM((SLOTS, nb * blk, blk), B16),
                pltpu.VMEM((HALF, HALF), F32),
                pltpu.VMEM((HALF, BLK), F32),
                dma((nb, nb)),
                dma((SLOTS, nb)),
                dma((SLOTS, nb)),
                dma((GRID - 1, nb)),
                dma((SLOTS, 2, nb)),
                dma((2,)),
                dma((GRID - 1, 2)),
                reg,
                reg((GRID - 1,)),
                reg((2,)),
            ],
            compiler_params=pltpu.CompilerParams(collective_id=0, has_side_effects=True, vmem_limit_bytes=56 * 1024 * 1024),
        )(a_loc)
        row_id = lax.axis_index("row")
        col_id = lax.axis_index("col")
        row_blk = jnp.arange(nb) * GRID + row_id
        col_blk = jnp.arange(width // blk) * GRID + col_id
        keep = row_blk[:, None, None, None] >= col_blk[None, None, :, None]
        return jnp.where(keep, work.reshape(nb, blk, width // blk, blk), 0.0).reshape(nb, blk, width)

    spec = P(("batch", "row"), None, "col")
    return jax.shard_map(factor_local, mesh=mesh, in_specs=(spec,), out_specs=spec, check_vma=False)
```

```python
import functools

import jax
import jax.numpy as jnp
from jax import lax
from jax.experimental import pallas as pl
from jax.experimental.pallas import tpu as pltpu
from jax.sharding import PartitionSpec as P

MESH = pl.DeviceIdType.MESH
HIGH = lax.Precision.HIGHEST
GRID = 4
BLK = 256
HALF = 128
PAN = 16
SLOTS = 4
F32, B16 = jnp.float32, jnp.bfloat16
NT = (((1,), (1,)), ((), ()))
TN = (((0,), (0,)), ((), ()))


def split3(x):
    hi = x.astype(B16)
    rest = x - hi.astype(F32)
    mid = rest.astype(B16)
    return hi, mid, (rest - mid.astype(F32)).astype(B16)


def gram(left, right):
    a1, a2, a3 = split3(left)
    b1, b2, b3 = split3(right)
    lhs = jnp.concatenate([a1, a1, a2, a2, a1, a3], axis=0)
    rhs = jnp.concatenate([b1, b2, b1, b2, b3, b1], axis=0)
    return lax.dot_general(lhs, rhs, TN, preferred_element_type=F32)


def eliminate(rows, base):
    groups = rows.shape[0]
    cols = [jnp.broadcast_to(rows[0][:, base + t : base + t + 1], (PAN, HALF))[None] for t in range(PAN)]
    work = jnp.concatenate(cols + [rows], axis=0)
    sub = lax.broadcasted_iota(jnp.int32, (PAN, HALF), 0)
    scale = jnp.zeros((PAN, HALF), F32)
    for t in range(PAN):
        root = jnp.broadcast_to(lax.rsqrt(work[0, t : t + 1, :]), (PAN, HALF))
        scale = jnp.where(sub == t, root, scale)
        mult = jnp.where(sub > t, work[0] * (root * root), 0.0)
        work = work[1:]
        work = work - mult[None] * work[:, t : t + 1, :]
    return work[-groups:] * scale[None]


def factor_half(tab, emit):
    count = HALF // PAN
    groups = tab.shape[1] // HALF
    done = []
    for p in range(count):
        own = tab[:PAN]
        rows = jnp.concatenate([own[None, :, g * HALF : (g + 1) * HALF] for g in range(groups)], axis=0)
        out = eliminate(rows, p * PAN)
        flat = jnp.concatenate([out[g] for g in range(groups)], axis=1)
        done.append(flat)
        emit(p, flat)
        if p + 1 < count:
            tab = tab[PAN:] - gram(flat[:, :HALF], flat)[(p + 1) * PAN :]
    return jnp.concatenate(done, axis=0)


def kernel(nb, a_ref, o_ref, mat, row_pan, col_pan, inv_a, inv_b, nxt_a, nxt_b, nxt_x, load_sem, br_recv, bc_recv,
           row_send, chain_send, inv_recv, inv_send, nxt_recv, x_recv, x_send, row_free, inv_free, chain_free, nxt_free, x_free):
    r = lax.axis_index("row")
    c = lax.axis_index("col")
    steps = nb * GRID
    last = GRID * (nb - 1)

    def first_block(k, pos):
        return lax.div(k + GRID - pos, GRID)

    def rows_of(t):
        return pl.ds(pl.multiple_of(t * BLK, BLK), BLK)

    def load(t, s):
        return pltpu.make_async_copy(a_ref.at[t, :, pl.ds(s * BLK, BLK)], mat.at[s, pl.ds(t * BLK, BLK), :], load_sem.at[t, s])

    def store(t, s):
        return pltpu.make_async_copy(mat.at[s, pl.ds(t * BLK, BLK), :], o_ref.at[t, :, pl.ds(pl.multiple_of(s * BLK, BLK), BLK)], load_sem.at[t, s])

    for s in range(nb):
        for t in range(nb):
            load(t, s).start()

    barrier = pltpu.get_barrier_semaphore()
    for off in range(1, GRID):
        pl.semaphore_signal(barrier, inc=1, device_id={"row": lax.rem(r + off, GRID)}, device_id_type=MESH)
        pl.semaphore_signal(barrier, inc=1, device_id={"col": lax.rem(c + off, GRID)}, device_id_type=MESH)
    for off in (1, GRID - 1):
        pl.semaphore_signal(barrier, inc=1, device_id={"row": lax.rem(r + off, GRID), "col": lax.rem(c + off, GRID)}, device_id_type=MESH)
    pl.semaphore_wait(barrier, 2 * GRID)

    for t in range(nb):
        load(t, 0).wait()

    def row_copy(slot, t, off):
        return pltpu.make_async_remote_copy(
            src_ref=row_pan.at[slot, rows_of(t), :], dst_ref=row_pan.at[slot, rows_of(t), :],
            send_sem=row_send.at[off - 1, t], recv_sem=br_recv.at[slot, t],
            device_id={"col": lax.rem(c + off, GRID)}, device_id_type=MESH)

    def chain_copy(src, slot, s, way):
        return pltpu.make_async_remote_copy(
            src_ref=src.at[slot, rows_of(s), :], dst_ref=col_pan.at[slot, rows_of(s), :],
            send_sem=chain_send.at[slot, way, s], recv_sem=bc_recv.at[slot, s],
            device_id={"row": r + 1 - 2 * way}, device_id_type=MESH)

    def inv_part(a, b, part):
        return a if part == 0 else b.at[pl.ds((part - 1) * (HALF // 2), HALF // 2), :]

    def inv_copy(off, part):
        ref = inv_part(inv_a, inv_b, part)
        return pltpu.make_async_remote_copy(
            src_ref=ref, dst_ref=ref, send_sem=inv_send.at[off, part], recv_sem=inv_recv.at[part],
            device_id={"row": lax.rem(r + off, GRID)}, device_id_type=MESH)

    def nxt_copy(part):
        return pltpu.make_async_remote_copy(
            src_ref=inv_part(inv_a, inv_b, part), dst_ref=inv_part(nxt_a, nxt_b, part),
            send_sem=inv_send.at[0, part], recv_sem=nxt_recv.at[part],
            device_id={"row": lax.rem(r + 1, GRID), "col": lax.rem(c + 1, GRID)}, device_id_type=MESH)

    def x_copy(k):
        return pltpu.make_async_remote_copy(
            src_ref=mat.at[lax.div(k, GRID), rows_of(lax.div(k + 1, GRID)), :], dst_ref=nxt_x,
            send_sem=x_send, recv_sem=x_recv,
            device_id={"col": lax.rem(c + 1, GRID)}, device_id_type=MESH)

    def gather_inv(a, b):
        return jnp.concatenate([jnp.concatenate([a[...], jnp.zeros((HALF, HALF), F32)], axis=1), b[...]], axis=0)

    def sends(way):
        return ((r >= c) & (r < GRID - 1)) if way == 0 else ((r <= c) & (r > 0))

    def pass_on(src, k, s):
        slot = lax.rem(k, SLOTS)
        for way in range(2):
            @pl.when(sends(way))
            def _():
                @pl.when((s == first_block(k, c)) & (k >= SLOTS))
                def _():
                    pl.semaphore_wait(chain_free.at[way], 1)
                chain_copy(src, slot, s, way).start()

    def own_col_block(k, s):
        slot = lax.rem(k, SLOTS)
        col_pan[slot, rows_of(s), :] = row_pan[slot, rows_of(s), :]
        pass_on(row_pan, k, s)

    def take_row(k, t):
        row_copy(lax.rem(k, SLOTS), t, 1).wait_recv()

        @pl.when(r == c)
        def _():
            own_col_block(k, t)

    def take_col(k, s):
        chain_copy(col_pan, lax.rem(k, SLOTS), s, 0).wait_recv()
        pass_on(col_pan, k, s)

    def update(k, t, s, count):
        slot = lax.rem(k, SLOTS)
        span = pl.ds(pl.multiple_of(t * BLK, BLK), count * BLK)
        prod = lax.dot_general(row_pan[slot, span, :], col_pan[slot, rows_of(s), :], NT, preferred_element_type=F32)
        mat[s, span, :] = mat[s, span, :] - prod

    def loop(lo, hi, body):
        def run(i, carry):
            body(i)
            return carry
        lax.fori_loop(lo, hi, run, 0)

    def factor_diag(k):
        t0 = lax.div(k, GRID)
        blk = mat[t0, rows_of(t0), :]
        eye = (lax.broadcasted_iota(jnp.int32, (HALF, HALF), 0) == lax.broadcasted_iota(jnp.int32, (HALF, HALF), 1)).astype(F32)

        def for_peers(act):
            for off in range(1, GRID):
                @pl.when(k < last + lax.rem(r + off, GRID))
                def _():
                    act(off)

        @pl.when(k >= GRID)
        def _():
            for_peers(lambda off: pl.semaphore_wait(inv_free.at[off - 1], 1))

            @pl.when(k + 1 < steps)
            def _():
                pl.semaphore_wait(nxt_free, 1)

        def send(part):
            @pl.when(k + 1 < steps)
            def _():
                nxt_copy(part).start()
            for_peers(lambda off: inv_copy(off, part).start())

        def emit_top(p, flat):
            inv_a[p * PAN : (p + 1) * PAN, :] = flat[:, 2 * HALF :]
            if p == HALF // PAN - 1:
                send(0)

        def emit_low(p, flat):
            inv_b[p * PAN : (p + 1) * PAN, :] = flat[:, HALF:]
            if (p + 1) % (HALF // PAN // 2) == 0:
                send(2 * (p + 1) // (HALF // PAN))

        top = factor_half(jnp.concatenate([blk[:HALF], eye], axis=1), emit_top)
        mid = lax.dot_general(top[:, HALF : 2 * HALF], top[:, HALF:], TN, precision=HIGH, preferred_element_type=F32)
        low = factor_half(jnp.concatenate([blk[HALF:, HALF:] - mid[:, :HALF], -mid[:, HALF:], eye], axis=1), emit_low)
        zero = jnp.zeros((HALF, HALF), F32)
        up = lax.broadcasted_iota(jnp.int32, (HALF, HALF), 0) <= lax.broadcasted_iota(jnp.int32, (HALF, HALF), 1)
        left = jnp.concatenate([jnp.where(up, top[:, :HALF], 0.0).T, top[:, HALF : 2 * HALF].T], axis=0)
        right = jnp.concatenate([zero, jnp.where(up, low[:, :HALF], 0.0).T], axis=0)
        mat[t0, rows_of(t0), :] = jnp.concatenate([left, right], axis=1)

    def for_row(k, t, act):
        @pl.when((r != lax.rem(k + 1, GRID)) | (t != lax.div(k + 1, GRID)))
        def _():
            act(1)
        for off in range(2, GRID):
            act(off)

    def solve_col(k):
        t0 = lax.div(k, GRID)
        slot = lax.rem(k, SLOTS)

        @pl.when(k < last + r)
        def _():
            @pl.when(r != c)
            def _():
                for part in range(3):
                    inv_copy(1, part).wait_recv()

            @pl.when(k >= SLOTS)
            def _():
                pl.semaphore_wait(row_free, GRID - 1)

        early = (r == lax.rem(k + 1, GRID)) & (k + 1 < steps)

        @pl.when(early)
        def _():
            x_copy(k).wait_send()

        def one(t):
            inv = gather_inv(inv_a, inv_b)
            sol = lax.dot_general(mat[t0, rows_of(t), :], inv, NT, precision=HIGH, preferred_element_type=F32)
            mat[t0, rows_of(t), :] = sol
            row_pan[slot, rows_of(t), :] = sol.astype(B16)
            for_row(k, t, lambda off: row_copy(slot, t, off).start())

            @pl.when(r == c)
            def _():
                own_col_block(k, t)

        loop(first_block(k, r), nb, one)

        @pl.when(r == c)
        def _():
            for off in range(1, GRID):
                @pl.when(k < last + lax.rem(r + off, GRID))
                def _():
                    for part in range(3):
                        inv_copy(off, part).wait_send()

            @pl.when(k + 1 < steps)
            def _():
                for part in range(3):
                    nxt_copy(part).wait_send()

        @pl.when((r != c) & (k + GRID < last + r))
        def _():
            pl.semaphore_signal(inv_free.at[lax.rem(r - c + GRID, GRID) - 1], inc=1, device_id={"row": lax.rem(k, GRID)}, device_id_type=MESH)

    def columns(k, lo, hi):
        def column(s):
            first = jnp.maximum(first_block(k, r), s)
            pairs = lax.div(nb - first, 2)
            loop(0, pairs, lambda q: update(k, first + 2 * q, s, 2))

            @pl.when(lax.rem(nb - first, 2) == 1)
            def _():
                update(k, nb - 1, s, 1)

        @pl.when(r != c)
        def _():
            loop(lo, hi, lambda s: take_col(k, s))
        loop(lo, hi, column)

    def trail(k):
        d = lax.rem(k, GRID)
        nxt = lax.rem(k + 1, GRID)
        soon = (c == lax.rem(k + 2, GRID)) & (k + 2 < steps)
        s_lo = first_block(k, c) + jnp.where(c == nxt, 1, 0)

        @pl.when((c != d) & (c != nxt))
        def _():
            loop(first_block(k, r), nb, lambda t: take_row(k, t))

        columns(k, s_lo, jnp.where(soon, s_lo + 1, nb))

    def finish(k):
        d = lax.rem(k, GRID)

        @pl.when(c == d)
        def _():
            for t in range(nb):
                store(t, lax.div(k, GRID)).start()

            def one(t):
                for_row(k, t, lambda off: row_copy(lax.rem(k, SLOTS), t, off).wait_send())
            loop(first_block(k, r), nb, one)

        for way in range(2):
            @pl.when(sends(way))
            def _():
                loop(first_block(k, c), nb, lambda s: chain_copy(col_pan, lax.rem(k, SLOTS), s, way).wait_send())

        @pl.when((c != d) & (k + SLOTS < last + r))
        def _():
            pl.semaphore_signal(row_free, inc=1, device_id={"col": d}, device_id_type=MESH)

        for way in range(2):
            @pl.when((k + SLOTS < last + c) & ((r > c) if way == 0 else (r < c)))
            def _():
                pl.semaphore_signal(chain_free.at[way], inc=1, device_id={"row": r - 1 + 2 * way}, device_id_type=MESH)

    def ahead(k):
        s1 = lax.div(k + 1, GRID)

        @pl.when(r == c)
        def _():
            slot = lax.rem(k, SLOTS)
            x_copy(k).wait_recv()
            for part in range(3):
                nxt_copy(part).wait_recv()
            sol = lax.dot_general(nxt_x[...], gather_inv(nxt_a, nxt_b), NT, precision=HIGH, preferred_element_type=F32).astype(B16)
            row_pan[slot, rows_of(s1), :] = sol
            col_pan[slot, rows_of(s1), :] = sol
            mat[s1, rows_of(s1), :] = mat[s1, rows_of(s1), :] - lax.dot_general(sol, sol, NT, preferred_element_type=F32)
            pass_on(row_pan, k, s1)

            @pl.when(k + GRID + 1 < steps)
            def _():
                pl.semaphore_signal(x_free, inc=1, device_id={"col": lax.rem(k, GRID)}, device_id_type=MESH)
                pl.semaphore_signal(nxt_free, inc=1, device_id={"row": lax.rem(k, GRID), "col": lax.rem(k, GRID)}, device_id_type=MESH)

        @pl.when(r != c)
        def _():
            take_col(k, s1)

            def one(t):
                take_row(k, t)
                update(k, t, s1, 1)

                @pl.when((r == lax.rem(k + 2, GRID)) & (t == lax.div(k + 2, GRID)) & (k + 2 < steps))
                def _():
                    @pl.when(k + 1 >= GRID)
                    def _():
                        pl.semaphore_wait(x_free, 1)
                    x_copy(k + 1).start()
            loop(first_block(k, r), nb, one)

    def ahead_rest(k):
        s1 = lax.div(k + 1, GRID)

        def one(t):
            take_row(k, t)
            update(k, t, s1, 1)
        loop(s1 + 1, nb, one)

    def step(k):
        d = lax.rem(k, GRID)

        @pl.when(c == d)
        def _():
            @pl.when(r == d)
            def _():
                factor_diag(k)

                @pl.when(k > 0)
                def _():
                    ahead_rest(k - 1)
            solve_col(k)

            @pl.when(k > 1)
            def _():
                columns(k - 2, lax.div(k, GRID) + 1, nb)

        @pl.when(k == 1)
        def _():
            for s in range(1, nb):
                for t in range(nb):
                    load(t, s).wait()

        @pl.when(k > 0)
        def _():
            trail(k - 1)

        @pl.when(k > 1)
        def _():
            finish(k - 2)

        @pl.when((c == lax.rem(k + 1, GRID)) & (k + 1 < steps))
        def _():
            ahead(k)

    @pl.when((r == 1) & (c == 0))
    def _():
        x_copy(0).start()

    loop(0, steps, step)
    finish(steps - 2)
    finish(steps - 1)

    for s in range(nb):
        for t in range(nb):
            store(t, s).wait()


def solution(mesh):
    def factor_local(a_loc):
        nb, blk, width = a_loc.shape
        dma = pltpu.SemaphoreType.DMA
        reg = pltpu.SemaphoreType.REGULAR
        work = pl.pallas_call(
            functools.partial(kernel, nb),
            out_shape=jax.ShapeDtypeStruct(a_loc.shape, F32),
            in_specs=[pl.BlockSpec(memory_space=pl.ANY)],
            out_specs=pl.BlockSpec(memory_space=pl.ANY),
            scratch_shapes=[
                pltpu.VMEM((nb, nb * blk, blk), F32),
                pltpu.VMEM((SLOTS, nb * blk, blk), B16),
                pltpu.VMEM((SLOTS, nb * blk, blk), B16),
                pltpu.VMEM((HALF, HALF), F32),
                pltpu.VMEM((HALF, BLK), F32),
                pltpu.VMEM((HALF, HALF), F32),
                pltpu.VMEM((HALF, BLK), F32),
                pltpu.VMEM((BLK, BLK), F32),
                dma((nb, nb)),
                dma((SLOTS, nb)),
                dma((SLOTS, nb)),
                dma((GRID - 1, nb)),
                dma((SLOTS, 2, nb)),
                dma((3,)),
                dma((GRID, 3)),
                dma((3,)),
                dma,
                dma,
                reg,
                reg((GRID - 1,)),
                reg((2,)),
                reg,
                reg,
            ],
            compiler_params=pltpu.CompilerParams(collective_id=0, has_side_effects=True, vmem_limit_bytes=56 * 1024 * 1024),
        )(a_loc)
        row_id = lax.axis_index("row")
        col_id = lax.axis_index("col")
        row_blk = jnp.arange(nb) * GRID + row_id
        col_blk = jnp.arange(width // blk) * GRID + col_id
        keep = row_blk[:, None, None, None] >= col_blk[None, None, :, None]
        return jnp.where(keep, work.reshape(nb, blk, width // blk, blk), 0.0).reshape(nb, blk, width)

    spec = P(("batch", "row"), None, "col")
    return jax.shard_map(factor_local, mesh=mesh, in_specs=(spec,), out_specs=spec, check_vma=False)
```

```python
import functools

import jax
import jax.numpy as jnp
from jax import lax
from jax.experimental import pallas as pl
from jax.experimental.pallas import tpu as pltpu
from jax.sharding import PartitionSpec as P

MESH = pl.DeviceIdType.MESH
HIGH = lax.Precision.HIGHEST
GRID = 4
BLK = 256
HALF = 128
PAN = 16
SLOTS = 4
F32, B16 = jnp.float32, jnp.bfloat16
NT = (((1,), (1,)), ((), ()))
TN = (((0,), (0,)), ((), ()))


def split3(x):
    hi = x.astype(B16)
    rest = x - hi.astype(F32)
    mid = rest.astype(B16)
    return hi, mid, (rest - mid.astype(F32)).astype(B16)


def gram(left, right):
    a1, a2, a3 = split3(left)
    b1, b2, b3 = split3(right)
    lhs = jnp.concatenate([a1, a1, a2, a2, a1, a3], axis=0)
    rhs = jnp.concatenate([b1, b2, b1, b2, b3, b1], axis=0)
    return lax.dot_general(lhs, rhs, TN, preferred_element_type=F32)


def eliminate(rows, base):
    groups = rows.shape[0]
    cols = [jnp.broadcast_to(rows[0][:, base + t : base + t + 1], (PAN, HALF))[None] for t in range(PAN)]
    work = jnp.concatenate(cols + [rows], axis=0)
    sub = lax.broadcasted_iota(jnp.int32, (PAN, HALF), 0)
    scale = jnp.zeros((PAN, HALF), F32)
    for t in range(PAN):
        root = jnp.broadcast_to(lax.rsqrt(work[0, t : t + 1, :]), (PAN, HALF))
        scale = jnp.where(sub == t, root, scale)
        mult = jnp.where(sub > t, work[0] * (root * root), 0.0)
        work = work[1:]
        work = work - mult[None] * work[:, t : t + 1, :]
    return work[-groups:] * scale[None]


def factor_half(tab, emit):
    count = HALF // PAN
    groups = tab.shape[1] // HALF
    done = []
    for p in range(count):
        own = tab[:PAN]
        rows = jnp.concatenate([own[None, :, g * HALF : (g + 1) * HALF] for g in range(groups)], axis=0)
        out = eliminate(rows, p * PAN)
        flat = jnp.concatenate([out[g] for g in range(groups)], axis=1)
        done.append(flat)
        emit(p, flat)
        if p + 1 < count:
            tab = tab[PAN:] - gram(flat[:, :HALF], flat)[(p + 1) * PAN :]
    return jnp.concatenate(done, axis=0)


def kernel(nb, a_ref, o_ref, mat, row_pan, col_pan, inv_a, inv_b, nxt_a, nxt_b, nxt_x, load_sem, br_recv, bc_recv,
           row_send, relay_send, chain_send, inv_recv, inv_send, nxt_recv, x_recv, x_send, row_free, inv_free, chain_free, nxt_free, x_free):
    r = lax.axis_index("row")
    c = lax.axis_index("col")
    steps = nb * GRID
    last = GRID * (nb - 1)

    def first_block(k, pos):
        return lax.div(k + GRID - pos, GRID)

    def rows_of(t):
        return pl.ds(pl.multiple_of(t * BLK, BLK), BLK)

    def load(t, s):
        return pltpu.make_async_copy(a_ref.at[t, :, pl.ds(s * BLK, BLK)], mat.at[s, pl.ds(t * BLK, BLK), :], load_sem.at[t, s])

    def store(t, s):
        return pltpu.make_async_copy(mat.at[s, pl.ds(t * BLK, BLK), :], o_ref.at[t, :, pl.ds(pl.multiple_of(s * BLK, BLK), BLK)], load_sem.at[t, s])

    for s in range(nb):
        for t in range(nb):
            load(t, s).start()

    barrier = pltpu.get_barrier_semaphore()
    for off in range(1, GRID):
        pl.semaphore_signal(barrier, inc=1, device_id={"row": lax.rem(r + off, GRID)}, device_id_type=MESH)
        pl.semaphore_signal(barrier, inc=1, device_id={"col": lax.rem(c + off, GRID)}, device_id_type=MESH)
    for off in (1, GRID - 1):
        pl.semaphore_signal(barrier, inc=1, device_id={"row": lax.rem(r + off, GRID), "col": lax.rem(c + off, GRID)}, device_id_type=MESH)
    pl.semaphore_wait(barrier, 2 * GRID)

    for t in range(nb):
        load(t, 0).wait()

    def row_copy(slot, t, off):
        return pltpu.make_async_remote_copy(
            src_ref=row_pan.at[slot, rows_of(t), :], dst_ref=row_pan.at[slot, rows_of(t), :],
            send_sem=row_send.at[off - 1, t], recv_sem=br_recv.at[slot, t],
            device_id={"col": lax.rem(c + off, GRID)}, device_id_type=MESH)

    def relay_copy(slot, t):
        return pltpu.make_async_remote_copy(
            src_ref=row_pan.at[slot, rows_of(t), :], dst_ref=row_pan.at[slot, rows_of(t), :],
            send_sem=relay_send.at[slot, t], recv_sem=br_recv.at[slot, t],
            device_id={"col": lax.rem(c + 1, GRID)}, device_id_type=MESH)

    def relays(k):
        return (lax.rem(c, 2) == 0) & (lax.div(c, 2) != lax.div(lax.rem(k, GRID), 2))

    def chain_copy(src, slot, s, way):
        return pltpu.make_async_remote_copy(
            src_ref=src.at[slot, rows_of(s), :], dst_ref=col_pan.at[slot, rows_of(s), :],
            send_sem=chain_send.at[slot, way, s], recv_sem=bc_recv.at[slot, s],
            device_id={"row": r + 1 - 2 * way}, device_id_type=MESH)

    def inv_part(a, b, part):
        return a if part == 0 else b.at[pl.ds((part - 1) * (HALF // 2), HALF // 2), :]

    def inv_copy(way, part):
        ref = inv_part(inv_a, inv_b, part)
        return pltpu.make_async_remote_copy(
            src_ref=ref, dst_ref=ref, send_sem=inv_send.at[1 + way, part], recv_sem=inv_recv.at[part],
            device_id={"row": r + 1 - 2 * way}, device_id_type=MESH)

    def inv_ways(k, act):
        for way in range(2):
            @pl.when(sends(way) & (k < last + r + 1 - 2 * way))
            def _():
                act(way)

    def nxt_copy(part):
        return pltpu.make_async_remote_copy(
            src_ref=inv_part(inv_a, inv_b, part), dst_ref=inv_part(nxt_a, nxt_b, part),
            send_sem=inv_send.at[0, part], recv_sem=nxt_recv.at[part],
            device_id={"row": lax.rem(r + 1, GRID), "col": lax.rem(c + 1, GRID)}, device_id_type=MESH)

    def x_copy(k):
        return pltpu.make_async_remote_copy(
            src_ref=mat.at[lax.div(k, GRID), rows_of(lax.div(k + 1, GRID)), :], dst_ref=nxt_x,
            send_sem=x_send, recv_sem=x_recv,
            device_id={"col": lax.rem(c + 1, GRID)}, device_id_type=MESH)

    def gather_inv(a, b):
        return jnp.concatenate([jnp.concatenate([a[...], jnp.zeros((HALF, HALF), F32)], axis=1), b[...]], axis=0)

    def sends(way):
        return ((r >= c) & (r < GRID - 1)) if way == 0 else ((r <= c) & (r > 0))

    def pass_on(src, k, s):
        slot = lax.rem(k, SLOTS)
        for way in range(2):
            @pl.when(sends(way))
            def _():
                @pl.when((s == first_block(k, c)) & (k >= SLOTS))
                def _():
                    pl.semaphore_wait(chain_free.at[way], 1)
                chain_copy(src, slot, s, way).start()

    def own_col_block(k, s):
        slot = lax.rem(k, SLOTS)
        col_pan[slot, rows_of(s), :] = row_pan[slot, rows_of(s), :]
        pass_on(row_pan, k, s)

    def take_row(k, t):
        row_copy(lax.rem(k, SLOTS), t, 1).wait_recv()

        @pl.when(relays(k))
        def _():
            relay_copy(lax.rem(k, SLOTS), t).start()

        @pl.when(r == c)
        def _():
            own_col_block(k, t)

    def take_col(k, s):
        chain_copy(col_pan, lax.rem(k, SLOTS), s, 0).wait_recv()
        pass_on(col_pan, k, s)

    def update(k, t, s, count):
        slot = lax.rem(k, SLOTS)
        span = pl.ds(pl.multiple_of(t * BLK, BLK), count * BLK)
        prod = lax.dot_general(row_pan[slot, span, :], col_pan[slot, rows_of(s), :], NT, preferred_element_type=F32)
        mat[s, span, :] = mat[s, span, :] - prod

    def loop(lo, hi, body):
        def run(i, carry):
            body(i)
            return carry
        lax.fori_loop(lo, hi, run, 0)

    def factor_diag(k):
        t0 = lax.div(k, GRID)
        blk = mat[t0, rows_of(t0), :]
        eye = (lax.broadcasted_iota(jnp.int32, (HALF, HALF), 0) == lax.broadcasted_iota(jnp.int32, (HALF, HALF), 1)).astype(F32)

        def for_peers(act):
            for off in range(1, GRID):
                @pl.when(k < last + lax.rem(r + off, GRID))
                def _():
                    act(off)

        @pl.when(k >= GRID)
        def _():
            for_peers(lambda off: pl.semaphore_wait(inv_free.at[off - 1], 1))

            @pl.when(k + 1 < steps)
            def _():
                pl.semaphore_wait(nxt_free, 1)

        def send(part):
            @pl.when(k + 1 < steps)
            def _():
                nxt_copy(part).start()
            inv_ways(k, lambda way: inv_copy(way, part).start())

        def emit_top(p, flat):
            inv_a[p * PAN : (p + 1) * PAN, :] = flat[:, 2 * HALF :]
            if p == HALF // PAN - 1:
                send(0)

        def emit_low(p, flat):
            inv_b[p * PAN : (p + 1) * PAN, :] = flat[:, HALF:]
            if (p + 1) % (HALF // PAN // 2) == 0:
                send(2 * (p + 1) // (HALF // PAN))

        top = factor_half(jnp.concatenate([blk[:HALF], eye], axis=1), emit_top)
        mid = lax.dot_general(top[:, HALF : 2 * HALF], top[:, HALF:], TN, precision=HIGH, preferred_element_type=F32)
        low = factor_half(jnp.concatenate([blk[HALF:, HALF:] - mid[:, :HALF], -mid[:, HALF:], eye], axis=1), emit_low)
        zero = jnp.zeros((HALF, HALF), F32)
        up = lax.broadcasted_iota(jnp.int32, (HALF, HALF), 0) <= lax.broadcasted_iota(jnp.int32, (HALF, HALF), 1)
        left = jnp.concatenate([jnp.where(up, top[:, :HALF], 0.0).T, top[:, HALF : 2 * HALF].T], axis=0)
        right = jnp.concatenate([zero, jnp.where(up, low[:, :HALF], 0.0).T], axis=0)
        mat[t0, rows_of(t0), :] = jnp.concatenate([left, right], axis=1)

    def for_row(k, t, act):
        own = (r == lax.rem(k + 1, GRID)) & (t == lax.div(k + 1, GRID))
        odd = lax.rem(c, 2)

        @pl.when(jnp.logical_not(own))
        def _():
            act(1)

        @pl.when(odd == 1)
        def _():
            act(3)

        @pl.when((odd == 0) | own)
        def _():
            act(2)

    def solve_col(k):
        t0 = lax.div(k, GRID)
        slot = lax.rem(k, SLOTS)

        @pl.when(k < last + r)
        def _():
            @pl.when(r != c)
            def _():
                for part in range(3):
                    inv_copy(0, part).wait_recv()
                    inv_ways(k, lambda way: inv_copy(way, part).start())

            @pl.when(k >= SLOTS)
            def _():
                pl.semaphore_wait(row_free, GRID - 1)

        early = (r == lax.rem(k + 1, GRID)) & (k + 1 < steps)

        @pl.when(early)
        def _():
            x_copy(k).wait_send()

        def one(t):
            @pl.when((k > 0) & ((t > first_block(k, r)) | (r == c)))
            def _():
                take_row(k - 1, t)
                update(k - 1, t, t0, 1)
            inv = gather_inv(inv_a, inv_b)
            sol = lax.dot_general(mat[t0, rows_of(t), :], inv, NT, precision=HIGH, preferred_element_type=F32)
            mat[t0, rows_of(t), :] = sol
            row_pan[slot, rows_of(t), :] = sol.astype(B16)
            for_row(k, t, lambda off: row_copy(slot, t, off).start())

            @pl.when(r == c)
            def _():
                own_col_block(k, t)

        loop(first_block(k, r), nb, one)

        @pl.when((k < last + r) | (r == c))
        def _():
            for part in range(3):
                inv_ways(k, lambda way: inv_copy(way, part).wait_send())

        @pl.when((r == c) & (k + 1 < steps))
        def _():
            for part in range(3):
                nxt_copy(part).wait_send()

        @pl.when((r != c) & (k + GRID < last + r))
        def _():
            pl.semaphore_signal(inv_free.at[lax.rem(r - c + GRID, GRID) - 1], inc=1, device_id={"row": lax.rem(k, GRID)}, device_id_type=MESH)

    def columns(k, lo, hi):
        def column(s):
            first = jnp.maximum(first_block(k, r), s)
            pairs = lax.div(nb - first, 2)
            loop(0, pairs, lambda q: update(k, first + 2 * q, s, 2))

            @pl.when(lax.rem(nb - first, 2) == 1)
            def _():
                update(k, nb - 1, s, 1)

        @pl.when(r != c)
        def _():
            loop(lo, hi, lambda s: take_col(k, s))
        loop(lo, hi, column)

    def trail(k):
        d = lax.rem(k, GRID)
        nxt = lax.rem(k + 1, GRID)
        soon = (c == lax.rem(k + 2, GRID)) & (k + 2 < steps)
        s_lo = first_block(k, c) + jnp.where(c == nxt, 1, 0)

        @pl.when((c != d) & (c != nxt))
        def _():
            loop(first_block(k, r), nb, lambda t: take_row(k, t))

        columns(k, s_lo, jnp.where(soon, s_lo + 1, nb))

    def finish(k):
        d = lax.rem(k, GRID)

        @pl.when(c == d)
        def _():
            for t in range(nb):
                store(t, lax.div(k, GRID)).start()

            def one(t):
                for_row(k, t, lambda off: row_copy(lax.rem(k, SLOTS), t, off).wait_send())
            loop(first_block(k, r), nb, one)

        @pl.when(relays(k))
        def _():
            made = (r == c) & (c == lax.rem(k + 1, GRID)) & (k + 1 < steps)
            loop(first_block(k, r) + jnp.where(made, 1, 0), nb, lambda t: relay_copy(lax.rem(k, SLOTS), t).wait_send())

        for way in range(2):
            @pl.when(sends(way))
            def _():
                loop(first_block(k, c), nb, lambda s: chain_copy(col_pan, lax.rem(k, SLOTS), s, way).wait_send())

        @pl.when((c != d) & (k + SLOTS < last + r))
        def _():
            pl.semaphore_signal(row_free, inc=1, device_id={"col": d}, device_id_type=MESH)

        for way in range(2):
            @pl.when((k + SLOTS < last + c) & ((r > c) if way == 0 else (r < c)))
            def _():
                pl.semaphore_signal(chain_free.at[way], inc=1, device_id={"row": r - 1 + 2 * way}, device_id_type=MESH)

    def ahead(k):
        s1 = lax.div(k + 1, GRID)

        @pl.when(r == c)
        def _():
            slot = lax.rem(k, SLOTS)
            x_copy(k).wait_recv()
            for part in range(3):
                nxt_copy(part).wait_recv()
            sol = lax.dot_general(nxt_x[...], gather_inv(nxt_a, nxt_b), NT, precision=HIGH, preferred_element_type=F32).astype(B16)
            row_pan[slot, rows_of(s1), :] = sol
            col_pan[slot, rows_of(s1), :] = sol
            mat[s1, rows_of(s1), :] = mat[s1, rows_of(s1), :] - lax.dot_general(sol, sol, NT, preferred_element_type=F32)
            pass_on(row_pan, k, s1)

            @pl.when(k + GRID + 1 < steps)
            def _():
                pl.semaphore_signal(x_free, inc=1, device_id={"col": lax.rem(k, GRID)}, device_id_type=MESH)
                pl.semaphore_signal(nxt_free, inc=1, device_id={"row": lax.rem(k, GRID), "col": lax.rem(k, GRID)}, device_id_type=MESH)

        @pl.when(r != c)
        def _():
            take_col(k, s1)

            t = first_block(k, r)

            @pl.when(t < nb)
            def _():
                take_row(k, t)
                update(k, t, s1, 1)

                @pl.when((r == lax.rem(k + 2, GRID)) & (k + 2 < steps))
                def _():
                    @pl.when(k + 1 >= GRID)
                    def _():
                        pl.semaphore_wait(x_free, 1)
                    x_copy(k + 1).start()

    def step(k):
        d = lax.rem(k, GRID)

        @pl.when(c == d)
        def _():
            @pl.when(r == d)
            def _():
                factor_diag(k)
            solve_col(k)

            @pl.when(k > 1)
            def _():
                columns(k - 2, lax.div(k, GRID) + 1, nb)

        @pl.when(k == 1)
        def _():
            for s in range(1, nb):
                for t in range(nb):
                    load(t, s).wait()

        @pl.when(k > 0)
        def _():
            trail(k - 1)

        @pl.when(k > 1)
        def _():
            finish(k - 2)

        @pl.when((c == lax.rem(k + 1, GRID)) & (k + 1 < steps))
        def _():
            ahead(k)

    @pl.when((r == 1) & (c == 0))
    def _():
        x_copy(0).start()

    loop(0, steps, step)
    finish(steps - 2)
    finish(steps - 1)

    for s in range(nb):
        for t in range(nb):
            store(t, s).wait()


def solution(mesh):
    def factor_local(a_loc):
        nb, blk, width = a_loc.shape
        dma = pltpu.SemaphoreType.DMA
        reg = pltpu.SemaphoreType.REGULAR
        work = pl.pallas_call(
            functools.partial(kernel, nb),
            out_shape=jax.ShapeDtypeStruct(a_loc.shape, F32),
            in_specs=[pl.BlockSpec(memory_space=pl.ANY)],
            out_specs=pl.BlockSpec(memory_space=pl.ANY),
            scratch_shapes=[
                pltpu.VMEM((nb, nb * blk, blk), F32),
                pltpu.VMEM((SLOTS, nb * blk, blk), B16),
                pltpu.VMEM((SLOTS, nb * blk, blk), B16),
                pltpu.VMEM((HALF, HALF), F32),
                pltpu.VMEM((HALF, BLK), F32),
                pltpu.VMEM((HALF, HALF), F32),
                pltpu.VMEM((HALF, BLK), F32),
                pltpu.VMEM((BLK, BLK), F32),
                dma((nb, nb)),
                dma((SLOTS, nb)),
                dma((SLOTS, nb)),
                dma((GRID - 1, nb)),
                dma((SLOTS, nb)),
                dma((SLOTS, 2, nb)),
                dma((3,)),
                dma((3, 3)),
                dma((3,)),
                dma,
                dma,
                reg,
                reg((GRID - 1,)),
                reg((2,)),
                reg,
                reg,
            ],
            compiler_params=pltpu.CompilerParams(collective_id=0, has_side_effects=True, vmem_limit_bytes=56 * 1024 * 1024),
        )(a_loc)
        row_id = lax.axis_index("row")
        col_id = lax.axis_index("col")
        row_blk = jnp.arange(nb) * GRID + row_id
        col_blk = jnp.arange(width // blk) * GRID + col_id
        keep = row_blk[:, None, None, None] >= col_blk[None, None, :, None]
        return jnp.where(keep, work.reshape(nb, blk, width // blk, blk), 0.0).reshape(nb, blk, width)

    spec = P(("batch", "row"), None, "col")
    return jax.shard_map(factor_local, mesh=mesh, in_specs=(spec,), out_specs=spec, check_vma=False)
```

```python
import functools

import jax
import jax.numpy as jnp
from jax import lax
from jax.experimental import pallas as pl
from jax.experimental.pallas import tpu as pltpu
from jax.sharding import PartitionSpec as P

MESH = pl.DeviceIdType.MESH
HIGH = lax.Precision.HIGHEST
GRID = 4
BLK = 256
HALF = 128
PAN = 16
SLOTS = 8
F32, B16 = jnp.float32, jnp.bfloat16
NT = (((1,), (1,)), ((), ()))
TN = (((0,), (0,)), ((), ()))


def split3(x):
    hi = x.astype(B16)
    rest = x - hi.astype(F32)
    mid = rest.astype(B16)
    return hi, mid, (rest - mid.astype(F32)).astype(B16)


def gram(left, right):
    a1, a2, a3 = split3(left)
    b1, b2, b3 = split3(right)
    lhs = jnp.concatenate([a1, a1, a2, a2, a1, a3], axis=0)
    rhs = jnp.concatenate([b1, b2, b1, b2, b3, b1], axis=0)
    return lax.dot_general(lhs, rhs, TN, preferred_element_type=F32)


def eliminate(rows, base):
    groups = rows.shape[0]
    cols = [jnp.broadcast_to(rows[0][:, base + t : base + t + 1], (PAN, HALF))[None] for t in range(PAN)]
    work = jnp.concatenate(cols + [rows], axis=0)
    sub = lax.broadcasted_iota(jnp.int32, (PAN, HALF), 0)
    scale = jnp.zeros((PAN, HALF), F32)
    for t in range(PAN):
        root = jnp.broadcast_to(lax.rsqrt(work[0, t : t + 1, :]), (PAN, HALF))
        scale = jnp.where(sub == t, root, scale)
        mult = jnp.where(sub > t, work[0] * (root * root), 0.0)
        work = work[1:]
        work = work - mult[None] * work[:, t : t + 1, :]
    return work[-groups:] * scale[None]


def factor_half(tab, emit):
    count = HALF // PAN
    groups = tab.shape[1] // HALF
    done = []
    for p in range(count):
        own = tab[:PAN]
        rows = jnp.concatenate([own[None, :, g * HALF : (g + 1) * HALF] for g in range(groups)], axis=0)
        out = eliminate(rows, p * PAN)
        flat = jnp.concatenate([out[g] for g in range(groups)], axis=1)
        done.append(flat)
        emit(p, flat)
        if p + 1 < count:
            tab = tab[PAN:] - gram(flat[:, :HALF], flat)[(p + 1) * PAN :]
    return jnp.concatenate(done, axis=0)


def kernel(nb, a_ref, o_ref, mat, row_pan, col_pan, inv_a, inv_b, nxt_a, nxt_b, nxt_x, load_sem, br_recv, bc_recv,
           row_send, relay_send, chain_send, inv_recv, inv_send, nxt_recv, x_recv, x_send, row_free, inv_free, chain_free, nxt_free, x_free):
    r = lax.axis_index("row")
    c = lax.axis_index("col")
    steps = nb * GRID
    last = GRID * (nb - 1)

    def first_block(k, pos):
        return lax.div(k + GRID - pos, GRID)

    def rows_of(t):
        return pl.ds(pl.multiple_of(t * BLK, BLK), BLK)

    def load(t, s):
        return pltpu.make_async_copy(a_ref.at[t, :, pl.ds(s * BLK, BLK)], mat.at[s, pl.ds(t * BLK, BLK), :], load_sem.at[t, s])

    def store(t, s):
        return pltpu.make_async_copy(mat.at[s, pl.ds(t * BLK, BLK), :], o_ref.at[t, :, pl.ds(pl.multiple_of(s * BLK, BLK), BLK)], load_sem.at[t, s])

    for s in range(nb):
        for t in range(nb):
            load(t, s).start()

    barrier = pltpu.get_barrier_semaphore()
    for off in range(1, GRID):
        pl.semaphore_signal(barrier, inc=1, device_id={"row": lax.rem(r + off, GRID)}, device_id_type=MESH)
        pl.semaphore_signal(barrier, inc=1, device_id={"col": lax.rem(c + off, GRID)}, device_id_type=MESH)
    for off in (1, GRID - 1):
        pl.semaphore_signal(barrier, inc=1, device_id={"row": lax.rem(r + off, GRID), "col": lax.rem(c + off, GRID)}, device_id_type=MESH)
    pl.semaphore_wait(barrier, 2 * GRID)

    for t in range(nb):
        load(t, 0).wait()

    def row_copy(slot, t, off):
        return pltpu.make_async_remote_copy(
            src_ref=row_pan.at[slot, rows_of(t), :], dst_ref=row_pan.at[slot, rows_of(t), :],
            send_sem=row_send.at[off - 1, t], recv_sem=br_recv.at[slot, t],
            device_id={"col": lax.rem(c + off, GRID)}, device_id_type=MESH)

    def relay_copy(slot, t):
        return pltpu.make_async_remote_copy(
            src_ref=row_pan.at[slot, rows_of(t), :], dst_ref=row_pan.at[slot, rows_of(t), :],
            send_sem=relay_send.at[slot, t], recv_sem=br_recv.at[slot, t],
            device_id={"col": lax.rem(c + 1, GRID)}, device_id_type=MESH)

    def relays(k):
        return (lax.rem(c, 2) == 0) & (lax.div(c, 2) != lax.div(lax.rem(k, GRID), 2))

    def chain_copy(src, slot, s, way):
        return pltpu.make_async_remote_copy(
            src_ref=src.at[slot, rows_of(s), :], dst_ref=col_pan.at[slot, rows_of(s), :],
            send_sem=chain_send.at[slot, way, s], recv_sem=bc_recv.at[slot, s],
            device_id={"row": r + 1 - 2 * way}, device_id_type=MESH)

    def inv_part(a, b, part):
        return a if part == 0 else b.at[pl.ds((part - 1) * (HALF // 2), HALF // 2), :]

    def inv_copy(way, part):
        ref = inv_part(inv_a, inv_b, part)
        return pltpu.make_async_remote_copy(
            src_ref=ref, dst_ref=ref, send_sem=inv_send.at[1 + way, part], recv_sem=inv_recv.at[part],
            device_id={"row": r + 1 - 2 * way}, device_id_type=MESH)

    def inv_ways(k, act):
        for way in range(2):
            @pl.when(sends(way) & (k < last + r + 1 - 2 * way))
            def _():
                act(way)

    def nxt_copy(part):
        return pltpu.make_async_remote_copy(
            src_ref=inv_part(inv_a, inv_b, part), dst_ref=inv_part(nxt_a, nxt_b, part),
            send_sem=inv_send.at[0, part], recv_sem=nxt_recv.at[part],
            device_id={"row": lax.rem(r + 1, GRID), "col": lax.rem(c + 1, GRID)}, device_id_type=MESH)

    def x_copy(k):
        return pltpu.make_async_remote_copy(
            src_ref=mat.at[lax.div(k, GRID), rows_of(lax.div(k + 1, GRID)), :], dst_ref=nxt_x,
            send_sem=x_send, recv_sem=x_recv,
            device_id={"col": lax.rem(c + 1, GRID)}, device_id_type=MESH)

    def gather_inv(a, b):
        return jnp.concatenate([jnp.concatenate([a[...], jnp.zeros((HALF, HALF), F32)], axis=1), b[...]], axis=0)

    def sends(way):
        return ((r >= c) & (r < GRID - 1)) if way == 0 else ((r <= c) & (r > 0))

    def pass_on(src, k, s):
        slot = lax.rem(k, SLOTS)
        for way in range(2):
            @pl.when(sends(way) & (s < nb - way))
            def _():
                @pl.when((s == first_block(k, c)) & (k >= SLOTS))
                def _():
                    pl.semaphore_wait(chain_free.at[way], 1)
                chain_copy(src, slot, s, way).start()

    def own_col_block(k, s):
        slot = lax.rem(k, SLOTS)
        col_pan[slot, rows_of(s), :] = row_pan[slot, rows_of(s), :]
        pass_on(row_pan, k, s)

    def take_row(k, t):
        row_copy(lax.rem(k, SLOTS), t, 1).wait_recv()

        @pl.when(relays(k))
        def _():
            relay_copy(lax.rem(k, SLOTS), t).start()

        @pl.when(r == c)
        def _():
            own_col_block(k, t)

    def take_col(k, s):
        chain_copy(col_pan, lax.rem(k, SLOTS), s, 0).wait_recv()
        pass_on(col_pan, k, s)

    def update(k, t, s, count):
        slot = lax.rem(k, SLOTS)
        span = pl.ds(pl.multiple_of(t * BLK, BLK), count * BLK)
        prod = lax.dot_general(row_pan[slot, span, :], col_pan[slot, rows_of(s), :], NT, preferred_element_type=F32)
        mat[s, span, :] = mat[s, span, :] - prod

    def loop(lo, hi, body):
        def run(i, carry):
            body(i)
            return carry
        lax.fori_loop(lo, hi, run, 0)

    def factor_diag(k):
        t0 = lax.div(k, GRID)
        blk = mat[t0, rows_of(t0), :]
        eye = (lax.broadcasted_iota(jnp.int32, (HALF, HALF), 0) == lax.broadcasted_iota(jnp.int32, (HALF, HALF), 1)).astype(F32)

        def for_peers(act):
            for off in range(1, GRID):
                @pl.when(k < last + lax.rem(r + off, GRID))
                def _():
                    act(off)

        @pl.when(k >= GRID)
        def _():
            for_peers(lambda off: pl.semaphore_wait(inv_free.at[off - 1], 1))

            @pl.when(k + 1 < steps)
            def _():
                pl.semaphore_wait(nxt_free, 1)

        def send(part):
            @pl.when(k + 1 < steps)
            def _():
                nxt_copy(part).start()
            inv_ways(k, lambda way: inv_copy(way, part).start())

        def emit_top(p, flat):
            inv_a[p * PAN : (p + 1) * PAN, :] = flat[:, 2 * HALF :]
            if p == HALF // PAN - 1:
                send(0)

        def emit_low(p, flat):
            inv_b[p * PAN : (p + 1) * PAN, :] = flat[:, HALF:]
            if (p + 1) % (HALF // PAN // 2) == 0:
                send(2 * (p + 1) // (HALF // PAN))

        top = factor_half(jnp.concatenate([blk[:HALF], eye], axis=1), emit_top)
        mid = lax.dot_general(top[:, HALF : 2 * HALF], top[:, HALF:], TN, precision=HIGH, preferred_element_type=F32)
        low = factor_half(jnp.concatenate([blk[HALF:, HALF:] - mid[:, :HALF], -mid[:, HALF:], eye], axis=1), emit_low)
        zero = jnp.zeros((HALF, HALF), F32)
        up = lax.broadcasted_iota(jnp.int32, (HALF, HALF), 0) <= lax.broadcasted_iota(jnp.int32, (HALF, HALF), 1)
        left = jnp.concatenate([jnp.where(up, top[:, :HALF], 0.0).T, top[:, HALF : 2 * HALF].T], axis=0)
        right = jnp.concatenate([zero, jnp.where(up, low[:, :HALF], 0.0).T], axis=0)
        mat[t0, rows_of(t0), :] = jnp.concatenate([left, right], axis=1)

    def for_row(k, t, act):
        own = (r == lax.rem(k + 1, GRID)) & (t == lax.div(k + 1, GRID))
        odd = lax.rem(c, 2)

        @pl.when(jnp.logical_not(own))
        def _():
            act(1)

        @pl.when(odd == 1)
        def _():
            act(3)

        @pl.when((odd == 0) | own)
        def _():
            act(2)

    def solve_col(k):
        t0 = lax.div(k, GRID)
        slot = lax.rem(k, SLOTS)

        @pl.when(k < last + r)
        def _():
            @pl.when(r != c)
            def _():
                for part in range(3):
                    inv_copy(0, part).wait_recv()
                    inv_ways(k, lambda way: inv_copy(way, part).start())

            @pl.when(k >= SLOTS)
            def _():
                pl.semaphore_wait(row_free.at[lax.rem(lax.div(k, GRID), SLOTS // GRID)], GRID - 1)

        early = (r == lax.rem(k + 1, GRID)) & (k + 1 < steps)

        @pl.when(early)
        def _():
            x_copy(k).wait_send()

        def one(t):
            @pl.when((k > 0) & ((t > first_block(k, r)) | (r == c)))
            def _():
                take_row(k - 1, t)
                update(k - 1, t, t0, 1)
            inv = gather_inv(inv_a, inv_b)
            sol = lax.dot_general(mat[t0, rows_of(t), :], inv, NT, precision=HIGH, preferred_element_type=F32)
            mat[t0, rows_of(t), :] = sol
            row_pan[slot, rows_of(t), :] = sol.astype(B16)
            for_row(k, t, lambda off: row_copy(slot, t, off).start())

            @pl.when(r == c)
            def _():
                own_col_block(k, t)

        loop(first_block(k, r), nb, one)

        @pl.when((k < last + r) | (r == c))
        def _():
            for part in range(3):
                inv_ways(k, lambda way: inv_copy(way, part).wait_send())

        @pl.when((r == c) & (k + 1 < steps))
        def _():
            for part in range(3):
                nxt_copy(part).wait_send()

        @pl.when((r != c) & (k + GRID < last + r))
        def _():
            pl.semaphore_signal(inv_free.at[lax.rem(r - c + GRID, GRID) - 1], inc=1, device_id={"row": lax.rem(k, GRID)}, device_id_type=MESH)

    top = nb - jnp.where(r < c, 1, 0)

    def columns(k, lo, hi):
        def column(s):
            first = jnp.maximum(first_block(k, r), s)
            pairs = lax.div(nb - first, 2)
            loop(0, pairs, lambda q: update(k, first + 2 * q, s, 2))

            @pl.when(lax.rem(nb - first, 2) == 1)
            def _():
                update(k, nb - 1, s, 1)

        @pl.when(r != c)
        def _():
            loop(lo, hi, lambda s: take_col(k, s))
        loop(lo, hi, column)

    def trail(k):
        d = lax.rem(k, GRID)
        nxt = lax.rem(k + 1, GRID)
        soon = (c == lax.rem(k + 2, GRID)) & (k + 2 < steps)
        s_lo = first_block(k, c) + jnp.where(c == nxt, 1, 0)

        @pl.when((c != d) & (c != nxt))
        def _():
            loop(first_block(k, r), nb, lambda t: take_row(k, t))

        columns(k, s_lo, jnp.where(soon, jnp.minimum(s_lo + 1, top), top))

    def finish(k):
        d = lax.rem(k, GRID)

        @pl.when(c == d)
        def _():
            for t in range(nb):
                store(t, lax.div(k, GRID)).start()

            def one(t):
                for_row(k, t, lambda off: row_copy(lax.rem(k, SLOTS), t, off).wait_send())
            loop(first_block(k, r), nb, one)

        @pl.when(relays(k))
        def _():
            made = (r == c) & (c == lax.rem(k + 1, GRID)) & (k + 1 < steps)
            loop(first_block(k, r) + jnp.where(made, 1, 0), nb, lambda t: relay_copy(lax.rem(k, SLOTS), t).wait_send())

        for way in range(2):
            @pl.when(sends(way))
            def _():
                loop(first_block(k, c), nb - way, lambda s: chain_copy(col_pan, lax.rem(k, SLOTS), s, way).wait_send())

        @pl.when((c != d) & (k + SLOTS < last + r))
        def _():
            pl.semaphore_signal(row_free.at[lax.rem(lax.div(k, GRID), SLOTS // GRID)], inc=1, device_id={"col": d}, device_id_type=MESH)

        for way in range(2):
            @pl.when((k + SLOTS < last - way * GRID + c) & ((r > c) if way == 0 else (r < c)))
            def _():
                pl.semaphore_signal(chain_free.at[way], inc=1, device_id={"row": r - 1 + 2 * way}, device_id_type=MESH)

    def ahead(k):
        s1 = lax.div(k + 1, GRID)

        @pl.when(r == c)
        def _():
            slot = lax.rem(k, SLOTS)
            x_copy(k).wait_recv()
            for part in range(3):
                nxt_copy(part).wait_recv()
            sol = lax.dot_general(nxt_x[...], gather_inv(nxt_a, nxt_b), NT, precision=HIGH, preferred_element_type=F32).astype(B16)
            row_pan[slot, rows_of(s1), :] = sol
            col_pan[slot, rows_of(s1), :] = sol
            mat[s1, rows_of(s1), :] = mat[s1, rows_of(s1), :] - lax.dot_general(sol, sol, NT, preferred_element_type=F32)
            pass_on(row_pan, k, s1)

            @pl.when(k + GRID + 1 < steps)
            def _():
                pl.semaphore_signal(x_free, inc=1, device_id={"col": lax.rem(k, GRID)}, device_id_type=MESH)
                pl.semaphore_signal(nxt_free, inc=1, device_id={"row": lax.rem(k, GRID), "col": lax.rem(k, GRID)}, device_id_type=MESH)

        @pl.when(r != c)
        def _():
            @pl.when(s1 < top)
            def _():
                take_col(k, s1)

            t = first_block(k, r)

            @pl.when(t < nb)
            def _():
                take_row(k, t)
                update(k, t, s1, 1)

                @pl.when((r == lax.rem(k + 2, GRID)) & (k + 2 < steps))
                def _():
                    @pl.when(k + 1 >= GRID)
                    def _():
                        pl.semaphore_wait(x_free, 1)
                    x_copy(k + 1).start()

    def step(k):
        d = lax.rem(k, GRID)

        @pl.when(c == d)
        def _():
            @pl.when(r == d)
            def _():
                factor_diag(k)
            solve_col(k)

            @pl.when(k > 1)
            def _():
                columns(k - 2, lax.div(k, GRID) + 1, top)

        @pl.when(k == 1)
        def _():
            for s in range(1, nb):
                for t in range(nb):
                    load(t, s).wait()

        @pl.when(k > 0)
        def _():
            trail(k - 1)

        @pl.when(k > 1)
        def _():
            finish(k - 2)

        @pl.when((c == lax.rem(k + 1, GRID)) & (k + 1 < steps))
        def _():
            ahead(k)

    @pl.when((r == 1) & (c == 0))
    def _():
        x_copy(0).start()

    loop(0, steps, step)
    finish(steps - 2)
    finish(steps - 1)

    for s in range(nb):
        for t in range(nb):
            store(t, s).wait()


def solution(mesh):
    def factor_local(a_loc):
        nb, blk, width = a_loc.shape
        dma = pltpu.SemaphoreType.DMA
        reg = pltpu.SemaphoreType.REGULAR
        work = pl.pallas_call(
            functools.partial(kernel, nb),
            out_shape=jax.ShapeDtypeStruct(a_loc.shape, F32),
            in_specs=[pl.BlockSpec(memory_space=pl.ANY)],
            out_specs=pl.BlockSpec(memory_space=pl.ANY),
            scratch_shapes=[
                pltpu.VMEM((nb, nb * blk, blk), F32),
                pltpu.VMEM((SLOTS, nb * blk, blk), B16),
                pltpu.VMEM((SLOTS, nb * blk, blk), B16),
                pltpu.VMEM((HALF, HALF), F32),
                pltpu.VMEM((HALF, BLK), F32),
                pltpu.VMEM((HALF, HALF), F32),
                pltpu.VMEM((HALF, BLK), F32),
                pltpu.VMEM((BLK, BLK), F32),
                dma((nb, nb)),
                dma((SLOTS, nb)),
                dma((SLOTS, nb)),
                dma((GRID - 1, nb)),
                dma((SLOTS, nb)),
                dma((SLOTS, 2, nb)),
                dma((3,)),
                dma((3, 3)),
                dma((3,)),
                dma,
                dma,
                reg((SLOTS // GRID,)),
                reg((GRID - 1,)),
                reg((2,)),
                reg,
                reg,
            ],
            compiler_params=pltpu.CompilerParams(collective_id=0, has_side_effects=True, vmem_limit_bytes=56 * 1024 * 1024),
        )(a_loc)
        row_id = lax.axis_index("row")
        col_id = lax.axis_index("col")
        row_blk = jnp.arange(nb) * GRID + row_id
        col_blk = jnp.arange(width // blk) * GRID + col_id
        keep = row_blk[:, None, None, None] >= col_blk[None, None, :, None]
        return jnp.where(keep, work.reshape(nb, blk, width // blk, blk), 0.0).reshape(nb, blk, width)

    spec = P(("batch", "row"), None, "col")
    return jax.shard_map(factor_local, mesh=mesh, in_specs=(spec,), out_specs=spec, check_vma=False)
```

```python
import functools

import jax
import jax.numpy as jnp
from jax import lax
from jax.experimental import pallas as pl
from jax.experimental.pallas import tpu as pltpu
from jax.sharding import PartitionSpec as P

MESH = pl.DeviceIdType.MESH
HIGH = lax.Precision.HIGHEST
GRID = 4
BLK = 256
HALF = 128
PAN = 16
SLOTS = 8
F32, B16 = jnp.float32, jnp.bfloat16
NT = (((1,), (1,)), ((), ()))
TN = (((0,), (0,)), ((), ()))


def split3(x):
    hi = x.astype(B16)
    rest = x - hi.astype(F32)
    mid = rest.astype(B16)
    return hi, mid, (rest - mid.astype(F32)).astype(B16)


def gram(left, right):
    a1, a2, a3 = split3(left)
    b1, b2, b3 = split3(right)
    lhs = jnp.concatenate([a1, a1, a2, a2, a1, a3], axis=0)
    rhs = jnp.concatenate([b1, b2, b1, b2, b3, b1], axis=0)
    return lax.dot_general(lhs, rhs, TN, preferred_element_type=F32)


def eliminate(rows, base):
    groups = rows.shape[0]
    cols = [jnp.broadcast_to(rows[0][:, base + t : base + t + 1], (PAN, HALF))[None] for t in range(PAN)]
    work = jnp.concatenate(cols + [rows], axis=0)
    sub = lax.broadcasted_iota(jnp.int32, (PAN, HALF), 0)
    scale = jnp.zeros((PAN, HALF), F32)
    for t in range(PAN):
        root = jnp.broadcast_to(lax.rsqrt(work[0, t : t + 1, :]), (PAN, HALF))
        scale = jnp.where(sub == t, root, scale)
        mult = jnp.where(sub > t, work[0] * (root * root), 0.0)
        work = work[1:]
        work = work - mult[None] * work[:, t : t + 1, :]
    return work[-groups:] * scale[None]


def factor_half(tab, emit):
    count = HALF // PAN
    groups = tab.shape[1] // HALF
    done = []
    for p in range(count):
        own = tab[:PAN]
        rows = jnp.concatenate([own[None, :, g * HALF : (g + 1) * HALF] for g in range(groups)], axis=0)
        out = eliminate(rows, p * PAN)
        flat = jnp.concatenate([out[g] for g in range(groups)], axis=1)
        done.append(flat)
        emit(p, flat)
        if p + 1 < count:
            tab = tab[PAN:] - gram(flat[:, :HALF], flat)[(p + 1) * PAN :]
    return jnp.concatenate(done, axis=0)


def kernel(nb, a_ref, o_ref, mat, row_pan, col_pan, inv_a, inv_b, nxt_a, nxt_b, nxt_x, nxt_y, x_out, load_sem, br_recv, bc_recv,
           row_send, relay_send, chain_send, inv_recv, inv_send, nxt_recv, x_recv, x_send, y_recv, y_send, row_free, inv_free, chain_free, nxt_free, x_free):
    r = lax.axis_index("row")
    c = lax.axis_index("col")
    steps = nb * GRID
    last = GRID * (nb - 1)

    def first_block(k, pos):
        return lax.div(k + GRID - pos, GRID)

    def rows_of(t):
        return pl.ds(pl.multiple_of(t * BLK, BLK), BLK)

    def load(t, s):
        return pltpu.make_async_copy(a_ref.at[t, :, pl.ds(s * BLK, BLK)], mat.at[s, pl.ds(t * BLK, BLK), :], load_sem.at[t, s])

    def store(t, s):
        return pltpu.make_async_copy(mat.at[s, pl.ds(t * BLK, BLK), :], o_ref.at[t, :, pl.ds(pl.multiple_of(s * BLK, BLK), BLK)], load_sem.at[t, s])

    for s in range(nb):
        for t in range(nb):
            load(t, s).start()

    barrier = pltpu.get_barrier_semaphore()
    for off in range(1, GRID):
        pl.semaphore_signal(barrier, inc=1, device_id={"row": lax.rem(r + off, GRID)}, device_id_type=MESH)
        pl.semaphore_signal(barrier, inc=1, device_id={"col": lax.rem(c + off, GRID)}, device_id_type=MESH)
    for off in (1, GRID - 1):
        pl.semaphore_signal(barrier, inc=1, device_id={"row": lax.rem(r + off, GRID), "col": lax.rem(c + off, GRID)}, device_id_type=MESH)
    pl.semaphore_wait(barrier, 2 * GRID)

    for t in range(nb):
        load(t, 0).wait()

    def row_copy(slot, t, off):
        return pltpu.make_async_remote_copy(
            src_ref=row_pan.at[slot, rows_of(t), :], dst_ref=row_pan.at[slot, rows_of(t), :],
            send_sem=row_send.at[off - 1, t], recv_sem=br_recv.at[slot, t],
            device_id={"col": lax.rem(c + off, GRID)}, device_id_type=MESH)

    def relay_copy(slot, t):
        return pltpu.make_async_remote_copy(
            src_ref=row_pan.at[slot, rows_of(t), :], dst_ref=row_pan.at[slot, rows_of(t), :],
            send_sem=relay_send.at[slot, t], recv_sem=br_recv.at[slot, t],
            device_id={"col": lax.rem(c + 1, GRID)}, device_id_type=MESH)

    def relays(k):
        return (lax.rem(c, 2) == 0) & (lax.div(c, 2) != lax.div(lax.rem(k, GRID), 2))

    def chain_copy(src, slot, s, way):
        return pltpu.make_async_remote_copy(
            src_ref=src.at[slot, rows_of(s), :], dst_ref=col_pan.at[slot, rows_of(s), :],
            send_sem=chain_send.at[slot, way, s], recv_sem=bc_recv.at[slot, s],
            device_id={"row": r + 1 - 2 * way}, device_id_type=MESH)

    def inv_part(a, b, part):
        return a if part == 0 else b.at[pl.ds((part - 1) * (HALF // 2), HALF // 2), :]

    def inv_copy(way, part):
        ref = inv_part(inv_a, inv_b, part)
        return pltpu.make_async_remote_copy(
            src_ref=ref, dst_ref=ref, send_sem=inv_send.at[1 + way, part], recv_sem=inv_recv.at[part],
            device_id={"row": r + 1 - 2 * way}, device_id_type=MESH)

    def inv_ways(k, act):
        for way in range(2):
            @pl.when(sends(way) & (k < last + r + 1 - 2 * way))
            def _():
                act(way)

    def nxt_copy(part):
        return pltpu.make_async_remote_copy(
            src_ref=inv_part(inv_a, inv_b, part), dst_ref=inv_part(nxt_a, nxt_b, part),
            send_sem=inv_send.at[0, part], recv_sem=nxt_recv.at[part],
            device_id={"row": lax.rem(r + 1, GRID), "col": lax.rem(c + 1, GRID)}, device_id_type=MESH)

    def x_copy(k):
        return pltpu.make_async_remote_copy(
            src_ref=x_out, dst_ref=nxt_x, send_sem=x_send, recv_sem=x_recv,
            device_id={"col": lax.rem(c + 1, GRID)}, device_id_type=MESH)

    def x_stage(k):
        x_out[...] = mat[lax.div(k, GRID), rows_of(lax.div(k + 1, GRID)), :]

    def y_copy(k):
        return pltpu.make_async_remote_copy(
            src_ref=row_pan.at[lax.rem(k, SLOTS), rows_of(lax.div(k + 1, GRID)), :], dst_ref=nxt_y,
            send_sem=y_send, recv_sem=y_recv,
            device_id={"row": lax.rem(r + 1, GRID), "col": lax.rem(c + 1, GRID)}, device_id_type=MESH)

    def gather_inv(a, b):
        return jnp.concatenate([jnp.concatenate([a[...], jnp.zeros((HALF, HALF), F32)], axis=1), b[...]], axis=0)

    def sends(way):
        return ((r >= c) & (r < GRID - 1)) if way == 0 else ((r <= c) & (r > 0))

    def pass_on(src, k, s):
        slot = lax.rem(k, SLOTS)
        for way in range(2):
            @pl.when(sends(way) & (s < nb - way))
            def _():
                @pl.when((s == first_block(k, c)) & (k >= SLOTS))
                def _():
                    pl.semaphore_wait(chain_free.at[way], 1)
                chain_copy(src, slot, s, way).start()

    def own_col_block(k, s):
        slot = lax.rem(k, SLOTS)
        col_pan[slot, rows_of(s), :] = row_pan[slot, rows_of(s), :]
        pass_on(row_pan, k, s)

    def take_row(k, t):
        row_copy(lax.rem(k, SLOTS), t, 1).wait_recv()

        @pl.when(relays(k))
        def _():
            relay_copy(lax.rem(k, SLOTS), t).start()

        @pl.when(r == c)
        def _():
            own_col_block(k, t)

    def take_col(k, s):
        chain_copy(col_pan, lax.rem(k, SLOTS), s, 0).wait_recv()
        pass_on(col_pan, k, s)

    def update(k, t, s, count):
        slot = lax.rem(k, SLOTS)
        span = pl.ds(pl.multiple_of(t * BLK, BLK), count * BLK)
        prod = lax.dot_general(row_pan[slot, span, :], col_pan[slot, rows_of(s), :], NT, preferred_element_type=F32)
        mat[s, span, :] = mat[s, span, :] - prod

    def loop(lo, hi, body):
        def run(i, carry):
            body(i)
            return carry
        lax.fori_loop(lo, hi, run, 0)

    def factor_diag(k):
        t0 = lax.div(k, GRID)
        blk = mat[t0, rows_of(t0), :]
        eye = (lax.broadcasted_iota(jnp.int32, (HALF, HALF), 0) == lax.broadcasted_iota(jnp.int32, (HALF, HALF), 1)).astype(F32)

        def for_peers(act):
            for off in range(1, GRID):
                @pl.when(k < last + lax.rem(r + off, GRID))
                def _():
                    act(off)

        @pl.when(k >= GRID)
        def _():
            for_peers(lambda off: pl.semaphore_wait(inv_free.at[off - 1], 1))

        def send(part):
            @pl.when(k + 1 < steps)
            def _():
                nxt_copy(part).start()
            inv_ways(k, lambda way: inv_copy(way, part).start())

        def emit_top(p, flat):
            inv_a[p * PAN : (p + 1) * PAN, :] = flat[:, 2 * HALF :]
            if p == HALF // PAN - 1:
                send(0)

        def emit_low(p, flat):
            inv_b[p * PAN : (p + 1) * PAN, :] = flat[:, HALF:]
            if (p + 1) % (HALF // PAN // 2) == 0:
                send(2 * (p + 1) // (HALF // PAN))

        top = factor_half(jnp.concatenate([blk[:HALF], eye], axis=1), emit_top)
        mid = lax.dot_general(top[:, HALF : 2 * HALF], top[:, HALF:], TN, precision=HIGH, preferred_element_type=F32)
        low = factor_half(jnp.concatenate([blk[HALF:, HALF:] - mid[:, :HALF], -mid[:, HALF:], eye], axis=1), emit_low)
        zero = jnp.zeros((HALF, HALF), F32)
        up = lax.broadcasted_iota(jnp.int32, (HALF, HALF), 0) <= lax.broadcasted_iota(jnp.int32, (HALF, HALF), 1)
        left = jnp.concatenate([jnp.where(up, top[:, :HALF], 0.0).T, top[:, HALF : 2 * HALF].T], axis=0)
        right = jnp.concatenate([zero, jnp.where(up, low[:, :HALF], 0.0).T], axis=0)
        mat[t0, rows_of(t0), :] = jnp.concatenate([left, right], axis=1)

    def for_row(k, t, act):
        own = (r == lax.rem(k + 1, GRID)) & (t == lax.div(k + 1, GRID))
        odd = lax.rem(c, 2)

        @pl.when(jnp.logical_not(own))
        def _():
            act(1)

        @pl.when(odd == 1)
        def _():
            act(3)

        @pl.when((odd == 0) | own)
        def _():
            act(2)

    def solve_col(k):
        t0 = lax.div(k, GRID)
        slot = lax.rem(k, SLOTS)

        @pl.when(k < last + r)
        def _():
            @pl.when(r != c)
            def _():
                for part in range(3):
                    inv_copy(0, part).wait_recv()
                    inv_ways(k, lambda way: inv_copy(way, part).start())

            @pl.when(k >= SLOTS)
            def _():
                pl.semaphore_wait(row_free.at[lax.rem(lax.div(k, GRID), SLOTS // GRID)], GRID - 1)

        early = (r == lax.rem(k + 1, GRID)) & (k + 1 < steps)

        @pl.when(early)
        def _():
            x_copy(k).wait_send()

        def one(t):
            @pl.when((k > 0) & ((t > first_block(k, r)) | (r == c)))
            def _():
                take_row(k - 1, t)
                update(k - 1, t, t0, 1)
            inv = gather_inv(inv_a, inv_b)
            sol = lax.dot_general(mat[t0, rows_of(t), :], inv, NT, precision=HIGH, preferred_element_type=F32)
            mat[t0, rows_of(t), :] = sol
            row_pan[slot, rows_of(t), :] = sol.astype(B16)
            for_row(k, t, lambda off: row_copy(slot, t, off).start())

            @pl.when(r == c)
            def _():
                own_col_block(k, t)

        loop(first_block(k, r), nb, one)

        @pl.when((k < last + r) | (r == c))
        def _():
            for part in range(3):
                inv_ways(k, lambda way: inv_copy(way, part).wait_send())

        @pl.when((r == c) & (k + 1 < steps))
        def _():
            for part in range(3):
                nxt_copy(part).wait_send()

            @pl.when(k > 0)
            def _():
                y_copy(k - 1).wait_send()

        @pl.when((r != c) & (k + GRID < last + r))
        def _():
            pl.semaphore_signal(inv_free.at[lax.rem(r - c + GRID, GRID) - 1], inc=1, device_id={"row": lax.rem(k, GRID)}, device_id_type=MESH)

    top = nb - jnp.where(r < c, 1, 0)

    def columns(k, lo, hi):
        def column(s):
            first = jnp.maximum(first_block(k, r), s)
            pairs = lax.div(nb - first, 2)
            loop(0, pairs, lambda q: update(k, first + 2 * q, s, 2))

            @pl.when(lax.rem(nb - first, 2) == 1)
            def _():
                update(k, nb - 1, s, 1)

        @pl.when(r != c)
        def _():
            loop(lo, hi, lambda s: take_col(k, s))
        loop(lo, hi, column)

    def trail(k):
        d = lax.rem(k, GRID)
        nxt = lax.rem(k + 1, GRID)
        soon = (c == lax.rem(k + 2, GRID)) & (k + 2 < steps)
        s_lo = first_block(k, c) + jnp.where(c == nxt, 1, 0)

        @pl.when((c != d) & (c != nxt))
        def _():
            loop(first_block(k, r), nb, lambda t: take_row(k, t))

        columns(k, s_lo, jnp.where(soon, jnp.minimum(s_lo + 1, top), top))

    def finish(k):
        d = lax.rem(k, GRID)

        @pl.when(c == d)
        def _():
            for t in range(nb):
                store(t, lax.div(k, GRID)).start()

            def one(t):
                for_row(k, t, lambda off: row_copy(lax.rem(k, SLOTS), t, off).wait_send())
            loop(first_block(k, r), nb, one)

        @pl.when(relays(k))
        def _():
            made = (r == c) & (c == lax.rem(k + 1, GRID)) & (k + 1 < steps)
            loop(first_block(k, r) + jnp.where(made, 1, 0), nb, lambda t: relay_copy(lax.rem(k, SLOTS), t).wait_send())

        for way in range(2):
            @pl.when(sends(way))
            def _():
                loop(first_block(k, c), nb - way, lambda s: chain_copy(col_pan, lax.rem(k, SLOTS), s, way).wait_send())

        @pl.when((c != d) & (k + SLOTS < last + r))
        def _():
            pl.semaphore_signal(row_free.at[lax.rem(lax.div(k, GRID), SLOTS // GRID)], inc=1, device_id={"col": d}, device_id_type=MESH)

        for way in range(2):
            @pl.when((k + SLOTS < last - way * GRID + c) & ((r > c) if way == 0 else (r < c)))
            def _():
                pl.semaphore_signal(chain_free.at[way], inc=1, device_id={"row": r - 1 + 2 * way}, device_id_type=MESH)

    def ahead(k):
        s1 = lax.div(k + 1, GRID)

        @pl.when(r == c)
        def _():
            slot = lax.rem(k, SLOTS)
            x_copy(k).wait_recv()

            @pl.when(k > 0)
            def _():
                y_copy(k - 1).wait_recv()
                prod = lax.dot_general(row_pan[lax.rem(k - 1 + SLOTS, SLOTS), rows_of(s1), :], nxt_y[...], NT, preferred_element_type=F32)
                nxt_x[...] = nxt_x[...] - prod
            for part in range(3):
                nxt_copy(part).wait_recv()
            sol = lax.dot_general(nxt_x[...], gather_inv(nxt_a, nxt_b), NT, precision=HIGH, preferred_element_type=F32).astype(B16)
            row_pan[slot, rows_of(s1), :] = sol
            col_pan[slot, rows_of(s1), :] = sol
            mat[s1, rows_of(s1), :] = mat[s1, rows_of(s1), :] - lax.dot_general(sol, sol, NT, preferred_element_type=F32)

            @pl.when(k + 2 < steps)
            def _():
                @pl.when(k + 1 >= GRID)
                def _():
                    pl.semaphore_wait(nxt_free, 1)
                y_copy(k).start()
            pass_on(row_pan, k, s1)

            @pl.when(k + GRID + 1 < steps)
            def _():
                pl.semaphore_signal(x_free, inc=1, device_id={"col": lax.rem(k, GRID)}, device_id_type=MESH)
                pl.semaphore_signal(nxt_free, inc=1, device_id={"row": lax.rem(k, GRID), "col": lax.rem(k, GRID)}, device_id_type=MESH)

        @pl.when(r != c)
        def _():
            @pl.when(s1 < top)
            def _():
                take_col(k, s1)

            t = first_block(k, r)

            @pl.when(t < nb)
            def _():
                take_row(k, t)
                update(k, t, s1, 1)

    def step(k):
        d = lax.rem(k, GRID)

        @pl.when(c == d)
        def _():
            @pl.when(r == d)
            def _():
                factor_diag(k)
            solve_col(k)

            @pl.when(k > 1)
            def _():
                columns(k - 2, lax.div(k, GRID) + 1, top)

        @pl.when(k == 1)
        def _():
            for s in range(1, nb):
                for t in range(nb):
                    load(t, s).wait()

        @pl.when(k > 0)
        def _():
            trail(k - 1)

        ready = (c == lax.rem(k + 1, GRID)) & (r == lax.rem(k + 2, GRID)) & (k + 2 < steps)

        @pl.when(ready)
        def _():
            x_stage(k + 1)

        @pl.when(k > 1)
        def _():
            finish(k - 2)

        @pl.when(ready)
        def _():
            @pl.when(k + 1 >= GRID)
            def _():
                pl.semaphore_wait(x_free, 1)
            x_copy(k + 1).start()

        @pl.when((c == lax.rem(k + 1, GRID)) & (k + 1 < steps))
        def _():
            ahead(k)

    @pl.when((r == 1) & (c == 0))
    def _():
        x_stage(0)
        x_copy(0).start()

    loop(0, steps, step)
    finish(steps - 2)
    finish(steps - 1)

    for s in range(nb):
        for t in range(nb):
            store(t, s).wait()


def solution(mesh):
    def factor_local(a_loc):
        nb, blk, width = a_loc.shape
        dma = pltpu.SemaphoreType.DMA
        reg = pltpu.SemaphoreType.REGULAR
        work = pl.pallas_call(
            functools.partial(kernel, nb),
            out_shape=jax.ShapeDtypeStruct(a_loc.shape, F32),
            in_specs=[pl.BlockSpec(memory_space=pl.ANY)],
            out_specs=pl.BlockSpec(memory_space=pl.ANY),
            scratch_shapes=[
                pltpu.VMEM((nb, nb * blk, blk), F32),
                pltpu.VMEM((SLOTS, nb * blk, blk), B16),
                pltpu.VMEM((SLOTS, nb * blk, blk), B16),
                pltpu.VMEM((HALF, HALF), F32),
                pltpu.VMEM((HALF, BLK), F32),
                pltpu.VMEM((HALF, HALF), F32),
                pltpu.VMEM((HALF, BLK), F32),
                pltpu.VMEM((BLK, BLK), F32),
                pltpu.VMEM((BLK, BLK), B16),
                pltpu.VMEM((BLK, BLK), F32),
                dma((nb, nb)),
                dma((SLOTS, nb)),
                dma((SLOTS, nb)),
                dma((GRID - 1, nb)),
                dma((SLOTS, nb)),
                dma((SLOTS, 2, nb)),
                dma((3,)),
                dma((3, 3)),
                dma((3,)),
                dma,
                dma,
                dma,
                dma,
                reg((SLOTS // GRID,)),
                reg((GRID - 1,)),
                reg((2,)),
                reg,
                reg,
            ],
            compiler_params=pltpu.CompilerParams(collective_id=0, has_side_effects=True, vmem_limit_bytes=36 * 1024 * 1024),
        )(a_loc)
        row_id = lax.axis_index("row")
        col_id = lax.axis_index("col")
        row_blk = jnp.arange(nb) * GRID + row_id
        col_blk = jnp.arange(width // blk) * GRID + col_id
        keep = row_blk[:, None, None, None] >= col_blk[None, None, :, None]
        return jnp.where(keep, work.reshape(nb, blk, width // blk, blk), 0.0).reshape(nb, blk, width)

    spec = P(("batch", "row"), None, "col")
    return jax.shard_map(factor_local, mesh=mesh, in_specs=(spec,), out_specs=spec, check_vma=False)
```

```python
import functools

import jax
import jax.numpy as jnp
from jax import lax
from jax.experimental import pallas as pl
from jax.experimental.pallas import tpu as pltpu
from jax.sharding import PartitionSpec as P

MESH = pl.DeviceIdType.MESH
HIGH = lax.Precision.HIGHEST
GRID = 4
BLK = 256
HALF = 128
PAN = 16
SLOTS = 8
F32, B16 = jnp.float32, jnp.bfloat16
NT = (((1,), (1,)), ((), ()))
TN = (((0,), (0,)), ((), ()))


def split3(x):
    hi = x.astype(B16)
    rest = x - hi.astype(F32)
    mid = rest.astype(B16)
    return hi, mid, (rest - mid.astype(F32)).astype(B16)


def gram(left, right):
    a1, a2, a3 = split3(left)
    b1, b2, b3 = split3(right)
    lhs = jnp.concatenate([a1, a1, a2, a2, a1, a3], axis=0)
    rhs = jnp.concatenate([b1, b2, b1, b2, b3, b1], axis=0)
    return lax.dot_general(lhs, rhs, TN, preferred_element_type=F32)


def eliminate(rows, base):
    groups = rows.shape[0]
    cols = [jnp.broadcast_to(rows[0][:, base + t : base + t + 1], (PAN, HALF))[None] for t in range(PAN)]
    work = jnp.concatenate(cols + [rows], axis=0)
    sub = lax.broadcasted_iota(jnp.int32, (PAN, HALF), 0)
    scale = jnp.zeros((PAN, HALF), F32)
    for t in range(PAN):
        root = jnp.broadcast_to(lax.rsqrt(work[0, t : t + 1, :]), (PAN, HALF))
        scale = jnp.where(sub == t, root, scale)
        mult = jnp.where(sub > t, work[0] * (root * root), 0.0)
        work = work[1:]
        work = work - mult[None] * work[:, t : t + 1, :]
    return work[-groups:] * scale[None]


def factor_half(tab, emit):
    count = HALF // PAN
    groups = tab.shape[1] // HALF
    done = []
    for p in range(count):
        own = tab[:PAN]
        rows = jnp.concatenate([own[None, :, g * HALF : (g + 1) * HALF] for g in range(groups)], axis=0)
        out = eliminate(rows, p * PAN)
        flat = jnp.concatenate([out[g] for g in range(groups)], axis=1)
        done.append(flat)
        emit(p, flat)
        if p + 1 < count:
            tab = tab[PAN:] - gram(flat[:, :HALF], flat)[(p + 1) * PAN :]
    return jnp.concatenate(done, axis=0)


def far_reach(nb):
    return 21 * nb // 8


def hist_at(t, nb):
    base = (far_reach(nb) + 1) // GRID
    m = t - base
    return m * (GRID * (base + 1) - 1 - far_reach(nb)) + m * (m - 1) * (GRID // 2)


def kernel(nb, a_ref, o_ref, mat, row_pan, col_pan, inv_a, inv_b, nxt_a, nxt_b, nxt_x, nxt_y, x_out, hist, far_col, load_sem, br_recv, bc_recv,
           row_send, relay_send, chain_send, inv_recv, inv_send, nxt_recv, x_recv, x_send, y_recv, y_send, row_free, inv_free, chain_free, nxt_free, x_free, far_recv, far_send,
           far_free):
    r = lax.axis_index("row")
    c = lax.axis_index("col")
    steps = nb * GRID
    last = GRID * (nb - 1)
    reach = far_reach(nb)
    base = (reach + 1) // GRID

    def first_block(k, pos):
        return lax.div(k + GRID - pos, GRID)

    def rows_of(t):
        return pl.ds(pl.multiple_of(t * BLK, BLK), BLK)

    def load(t, s):
        return pltpu.make_async_copy(a_ref.at[t, :, pl.ds(s * BLK, BLK)], mat.at[s, pl.ds(t * BLK, BLK), :], load_sem.at[t, s])

    def store(t, s):
        return pltpu.make_async_copy(mat.at[s, pl.ds(t * BLK, BLK), :], o_ref.at[t, :, pl.ds(pl.multiple_of(s * BLK, BLK), BLK)], load_sem.at[t, s])

    for s in range(nb):
        for t in range(nb):
            load(t, s).start()

    barrier = pltpu.get_barrier_semaphore()
    for off in range(1, GRID):
        pl.semaphore_signal(barrier, inc=1, device_id={"row": lax.rem(r + off, GRID)}, device_id_type=MESH)
        pl.semaphore_signal(barrier, inc=1, device_id={"col": lax.rem(c + off, GRID)}, device_id_type=MESH)
    for off in (1, GRID - 1):
        pl.semaphore_signal(barrier, inc=1, device_id={"row": lax.rem(r + off, GRID), "col": lax.rem(c + off, GRID)}, device_id_type=MESH)
    pl.semaphore_wait(barrier, 2 * GRID)

    for t in range(nb):
        load(t, 0).wait()

    def row_copy(slot, t, off):
        return pltpu.make_async_remote_copy(
            src_ref=row_pan.at[slot, rows_of(t), :], dst_ref=row_pan.at[slot, rows_of(t), :],
            send_sem=row_send.at[off - 1, t], recv_sem=br_recv.at[slot, t],
            device_id={"col": lax.rem(c + off, GRID)}, device_id_type=MESH)

    def relay_copy(slot, t):
        return pltpu.make_async_remote_copy(
            src_ref=row_pan.at[slot, rows_of(t), :], dst_ref=row_pan.at[slot, rows_of(t), :],
            send_sem=relay_send.at[slot, t], recv_sem=br_recv.at[slot, t],
            device_id={"col": lax.rem(c + 1, GRID)}, device_id_type=MESH)

    def relays(k):
        return (lax.rem(c, 2) == 0) & (lax.div(c, 2) != lax.div(lax.rem(k, GRID), 2))

    def chain_copy(src, slot, s, way):
        return pltpu.make_async_remote_copy(
            src_ref=src.at[slot, rows_of(s), :], dst_ref=col_pan.at[slot, rows_of(s), :],
            send_sem=chain_send.at[slot, way, s], recv_sem=bc_recv.at[slot, s],
            device_id={"row": r + 1 - 2 * way}, device_id_type=MESH)

    def inv_part(a, b, part):
        return a if part == 0 else b.at[pl.ds((part - 1) * (HALF // 2), HALF // 2), :]

    def inv_copy(way, part):
        ref = inv_part(inv_a, inv_b, part)
        return pltpu.make_async_remote_copy(
            src_ref=ref, dst_ref=ref, send_sem=inv_send.at[1 + way, part], recv_sem=inv_recv.at[part],
            device_id={"row": r + 1 - 2 * way}, device_id_type=MESH)

    def inv_ways(k, act):
        for way in range(2):
            @pl.when(sends(way) & (k < last + r + 1 - 2 * way))
            def _():
                act(way)

    def nxt_copy(part):
        return pltpu.make_async_remote_copy(
            src_ref=inv_part(inv_a, inv_b, part), dst_ref=inv_part(nxt_a, nxt_b, part),
            send_sem=inv_send.at[0, part], recv_sem=nxt_recv.at[part],
            device_id={"row": lax.rem(r + 1, GRID), "col": lax.rem(c + 1, GRID)}, device_id_type=MESH)

    def x_copy(k):
        return pltpu.make_async_remote_copy(
            src_ref=x_out, dst_ref=nxt_x, send_sem=x_send, recv_sem=x_recv,
            device_id={"col": lax.rem(c + 1, GRID)}, device_id_type=MESH)

    def x_stage(k):
        x_out[...] = mat[lax.div(k, GRID), rows_of(lax.div(k + 1, GRID)), :]

    def y_copy(k):
        return pltpu.make_async_remote_copy(
            src_ref=row_pan.at[lax.rem(k, SLOTS), rows_of(lax.div(k + 1, GRID)), :], dst_ref=nxt_y,
            send_sem=y_send, recv_sem=y_recv,
            device_id={"row": lax.rem(r + 1, GRID), "col": lax.rem(c + 1, GRID)}, device_id_type=MESH)

    def gather_inv(a, b):
        return jnp.concatenate([jnp.concatenate([a[...], jnp.zeros((HALF, HALF), F32)], axis=1), b[...]], axis=0)

    def sends(way):
        return ((r >= c) & (r < GRID - 1)) if way == 0 else ((r <= c) & (r > 0))

    def near(k):
        return jnp.minimum(nb, lax.div(k + reach - c, GRID) + 1)

    def pass_on(src, k, s):
        slot = lax.rem(k, SLOTS)
        for way in range(2):
            @pl.when(sends(way) & (s < jnp.minimum(near(k), nb - way)))
            def _():
                @pl.when((s == first_block(k, c)) & (k >= SLOTS))
                def _():
                    pl.semaphore_wait(chain_free.at[way], 1)
                chain_copy(src, slot, s, way).start()

    def own_col_block(k, s):
        slot = lax.rem(k, SLOTS)
        col_pan[slot, rows_of(s), :] = row_pan[slot, rows_of(s), :]
        pass_on(row_pan, k, s)

    def take_row(k, t):
        row_copy(lax.rem(k, SLOTS), t, 1).wait_recv()

        @pl.when(relays(k))
        def _():
            relay_copy(lax.rem(k, SLOTS), t).start()

        @pl.when(r == c)
        def _():
            own_col_block(k, t)

    def take_col(k, s):
        chain_copy(col_pan, lax.rem(k, SLOTS), s, 0).wait_recv()
        pass_on(col_pan, k, s)

    def update(k, t, s, count):
        slot = lax.rem(k, SLOTS)
        span = pl.ds(pl.multiple_of(t * BLK, BLK), count * BLK)
        prod = lax.dot_general(row_pan[slot, span, :], col_pan[slot, rows_of(s), :], NT, preferred_element_type=F32)
        mat[s, span, :] = mat[s, span, :] - prod

    def loop(lo, hi, body):
        def run(i, carry):
            body(i)
            return carry
        lax.fori_loop(lo, hi, run, 0)

    def factor_diag(k):
        t0 = lax.div(k, GRID)
        blk = mat[t0, rows_of(t0), :]
        eye = (lax.broadcasted_iota(jnp.int32, (HALF, HALF), 0) == lax.broadcasted_iota(jnp.int32, (HALF, HALF), 1)).astype(F32)

        def for_peers(act):
            for off in range(1, GRID):
                @pl.when(k < last + lax.rem(r + off, GRID))
                def _():
                    act(off)

        @pl.when(k >= GRID)
        def _():
            for_peers(lambda off: pl.semaphore_wait(inv_free.at[off - 1], 1))

        def send(part):
            @pl.when(k + 1 < steps)
            def _():
                nxt_copy(part).start()
            inv_ways(k, lambda way: inv_copy(way, part).start())

        def emit_top(p, flat):
            inv_a[p * PAN : (p + 1) * PAN, :] = flat[:, 2 * HALF :]
            if p == HALF // PAN - 1:
                send(0)

        def emit_low(p, flat):
            inv_b[p * PAN : (p + 1) * PAN, :] = flat[:, HALF:]
            if (p + 1) % (HALF // PAN // 2) == 0:
                send(2 * (p + 1) // (HALF // PAN))

        top = factor_half(jnp.concatenate([blk[:HALF], eye], axis=1), emit_top)
        mid = lax.dot_general(top[:, HALF : 2 * HALF], top[:, HALF:], TN, precision=HIGH, preferred_element_type=F32)
        low = factor_half(jnp.concatenate([blk[HALF:, HALF:] - mid[:, :HALF], -mid[:, HALF:], eye], axis=1), emit_low)
        zero = jnp.zeros((HALF, HALF), F32)
        up = lax.broadcasted_iota(jnp.int32, (HALF, HALF), 0) <= lax.broadcasted_iota(jnp.int32, (HALF, HALF), 1)
        left = jnp.concatenate([jnp.where(up, top[:, :HALF], 0.0).T, top[:, HALF : 2 * HALF].T], axis=0)
        right = jnp.concatenate([zero, jnp.where(up, low[:, :HALF], 0.0).T], axis=0)
        mat[t0, rows_of(t0), :] = jnp.concatenate([left, right], axis=1)

    def for_row(k, t, act):
        own = (r == lax.rem(k + 1, GRID)) & (t == lax.div(k + 1, GRID))
        odd = lax.rem(c, 2)

        @pl.when(jnp.logical_not(own))
        def _():
            act(1)

        @pl.when(odd == 1)
        def _():
            act(3)

        @pl.when((odd == 0) | own)
        def _():
            act(2)

    def solve_col(k):
        t0 = lax.div(k, GRID)
        slot = lax.rem(k, SLOTS)

        @pl.when(k < last + r)
        def _():
            @pl.when(r != c)
            def _():
                for part in range(3):
                    inv_copy(0, part).wait_recv()
                    inv_ways(k, lambda way: inv_copy(way, part).start())

            @pl.when(k >= SLOTS)
            def _():
                pl.semaphore_wait(row_free.at[lax.rem(lax.div(k, GRID), SLOTS // GRID)], GRID - 1)

        early = (r == lax.rem(k + 1, GRID)) & (k + 1 < steps)

        @pl.when(early)
        def _():
            x_copy(k).wait_send()

        def one(t):
            @pl.when((k > 0) & ((t > first_block(k, r)) | (r == c)))
            def _():
                take_row(k - 1, t)
                update(k - 1, t, t0, 1)
            inv = gather_inv(inv_a, inv_b)
            sol = lax.dot_general(mat[t0, rows_of(t), :], inv, NT, precision=HIGH, preferred_element_type=F32)
            mat[t0, rows_of(t), :] = sol
            row_pan[slot, rows_of(t), :] = sol.astype(B16)
            for_row(k, t, lambda off: row_copy(slot, t, off).start())

            @pl.when(r == c)
            def _():
                own_col_block(k, t)

        loop(first_block(k, r), nb, one)

        @pl.when((k < last + r) | (r == c))
        def _():
            for part in range(3):
                inv_ways(k, lambda way: inv_copy(way, part).wait_send())

        @pl.when((r == c) & (k + 1 < steps))
        def _():
            for part in range(3):
                nxt_copy(part).wait_send()

            @pl.when(k > 0)
            def _():
                y_copy(k - 1).wait_send()

        @pl.when((r != c) & (k + GRID < last + r))
        def _():
            pl.semaphore_signal(inv_free.at[lax.rem(r - c + GRID, GRID) - 1], inc=1, device_id={"row": lax.rem(k, GRID)}, device_id_type=MESH)

    top = nb - jnp.where(r < c, 1, 0)

    def columns(k, lo, hi):
        def column(s):
            first = jnp.maximum(first_block(k, r), s)
            pairs = lax.div(nb - first, 2)
            loop(0, pairs, lambda q: update(k, first + 2 * q, s, 2))

            @pl.when(lax.rem(nb - first, 2) == 1)
            def _():
                update(k, nb - 1, s, 1)

        @pl.when(r != c)
        def _():
            loop(lo, hi, lambda s: take_col(k, s))
        loop(lo, hi, column)

    def trail(k):
        d = lax.rem(k, GRID)
        nxt = lax.rem(k + 1, GRID)
        soon = (c == lax.rem(k + 2, GRID)) & (k + 2 < steps)
        s_lo = first_block(k, c) + jnp.where(c == nxt, 1, 0)

        @pl.when((c != d) & (c != nxt))
        def _():
            loop(first_block(k, r), nb, lambda t: take_row(k, t))

        @pl.when(k < steps - 1 - reach)
        def _():
            for t in range(base, nb):
                @pl.when(k < GRID * t + GRID - 1 - reach)
                def _():
                    hist[hist_at(t, nb) + k] = row_pan[lax.rem(k, SLOTS), t * BLK : (t + 1) * BLK, :]

        hi = jnp.minimum(top, near(k))
        columns(k, s_lo, jnp.where(soon, jnp.minimum(s_lo + 1, hi), hi))

    def far_copy(src, kp, way):
        return pltpu.make_async_remote_copy(
            src_ref=src, dst_ref=far_col.at[kp], send_sem=far_send.at[kp, way], recv_sem=far_recv.at[kp],
            device_id={"row": r + 1 - 2 * way}, device_id_type=MESH)

    def far_sent(j, way):
        return (j > reach) & (j < steps) & (lax.div(j, GRID) < nb - way)

    def far_pass(src, j, kp):
        for way in range(2):
            @pl.when(sends(way) & far_sent(j, way))
            def _():
                @pl.when((kp == 0) & (j - GRID > reach))
                def _():
                    pl.semaphore_wait(far_free.at[way], 1)
                far_copy(src, kp, way).start()

    def far_start(j):
        @pl.when((r == c) & (c == lax.rem(j, GRID)) & (j > reach) & (j < steps))
        def _():
            loop(0, j - reach, lambda kp: far_pass(hist.at[hist_at(lax.div(j, GRID), nb) + kp], j, kp))

    def far_take(j):
        s = lax.div(j, GRID)

        @pl.when((c == lax.rem(j, GRID)) & (j > reach) & (j < steps) & (s < top))
        def _():
            def one(kp):
                @pl.when(r == c)
                def _():
                    far_col[kp] = hist[hist_at(s, nb) + kp]

                @pl.when(r != c)
                def _():
                    far_copy(far_col.at[kp], kp, 0).wait_recv()
                    far_pass(far_col.at[kp], j, kp)

                def tile(t):
                    prod = lax.dot_general(hist[hist_at(t, nb) + kp], far_col[kp], NT, preferred_element_type=F32)
                    mat[s, rows_of(t), :] = mat[s, rows_of(t), :] - prod
                loop(s + jnp.where(r < c, 1, 0), nb, tile)
            loop(0, j - reach, one)

    def far_done(j):
        @pl.when((c == lax.rem(j, GRID)) & (j > reach) & (j < steps))
        def _():
            for way in range(2):
                @pl.when(sends(way) & far_sent(j, way))
                def _():
                    loop(0, j - reach, lambda kp: far_copy(far_col.at[kp], kp, way).wait_send())

                @pl.when(far_sent(j + GRID, way) & ((r > c) if way == 0 else (r < c)))
                def _():
                    pl.semaphore_signal(far_free.at[way], inc=1, device_id={"row": r - 1 + 2 * way}, device_id_type=MESH)

    def finish(k):
        d = lax.rem(k, GRID)

        @pl.when(c == d)
        def _():
            for t in range(nb):
                store(t, lax.div(k, GRID)).start()

            def one(t):
                for_row(k, t, lambda off: row_copy(lax.rem(k, SLOTS), t, off).wait_send())
            loop(first_block(k, r), nb, one)

        @pl.when(relays(k))
        def _():
            made = (r == c) & (c == lax.rem(k + 1, GRID)) & (k + 1 < steps)
            loop(first_block(k, r) + jnp.where(made, 1, 0), nb, lambda t: relay_copy(lax.rem(k, SLOTS), t).wait_send())

        for way in range(2):
            @pl.when(sends(way))
            def _():
                loop(first_block(k, c), jnp.minimum(near(k), nb - way), lambda s: chain_copy(col_pan, lax.rem(k, SLOTS), s, way).wait_send())

        @pl.when((c != d) & (k + SLOTS < last + r))
        def _():
            pl.semaphore_signal(row_free.at[lax.rem(lax.div(k, GRID), SLOTS // GRID)], inc=1, device_id={"col": d}, device_id_type=MESH)

        for way in range(2):
            @pl.when((k + SLOTS < last - way * GRID + c) & ((r > c) if way == 0 else (r < c)))
            def _():
                pl.semaphore_signal(chain_free.at[way], inc=1, device_id={"row": r - 1 + 2 * way}, device_id_type=MESH)

    def ahead(k):
        s1 = lax.div(k + 1, GRID)

        @pl.when(r == c)
        def _():
            slot = lax.rem(k, SLOTS)
            x_copy(k).wait_recv()

            @pl.when(k > 0)
            def _():
                y_copy(k - 1).wait_recv()
                prod = lax.dot_general(row_pan[lax.rem(k - 1 + SLOTS, SLOTS), rows_of(s1), :], nxt_y[...], NT, preferred_element_type=F32)
                nxt_x[...] = nxt_x[...] - prod
            for part in range(3):
                nxt_copy(part).wait_recv()
            sol = lax.dot_general(nxt_x[...], gather_inv(nxt_a, nxt_b), NT, precision=HIGH, preferred_element_type=F32).astype(B16)
            row_pan[slot, rows_of(s1), :] = sol
            col_pan[slot, rows_of(s1), :] = sol
            mat[s1, rows_of(s1), :] = mat[s1, rows_of(s1), :] - lax.dot_general(sol, sol, NT, preferred_element_type=F32)

            @pl.when(k + 2 < steps)
            def _():
                @pl.when(k + 1 >= GRID)
                def _():
                    pl.semaphore_wait(nxt_free, 1)
                y_copy(k).start()
            pass_on(row_pan, k, s1)

            @pl.when(k + GRID + 1 < steps)
            def _():
                pl.semaphore_signal(x_free, inc=1, device_id={"col": lax.rem(k, GRID)}, device_id_type=MESH)
                pl.semaphore_signal(nxt_free, inc=1, device_id={"row": lax.rem(k, GRID), "col": lax.rem(k, GRID)}, device_id_type=MESH)

        @pl.when(r != c)
        def _():
            @pl.when(s1 < top)
            def _():
                take_col(k, s1)

            t = first_block(k, r)

            @pl.when(t < nb)
            def _():
                take_row(k, t)
                update(k, t, s1, 1)

    def step(k):
        d = lax.rem(k, GRID)

        @pl.when(c == d)
        def _():
            @pl.when(r == d)
            def _():
                factor_diag(k)
            solve_col(k)

            @pl.when(k > 1)
            def _():
                columns(k - 2, lax.div(k, GRID) + 1, jnp.minimum(top, near(k - 2)))

        @pl.when(k == 1)
        def _():
            for s in range(1, nb):
                for t in range(nb):
                    load(t, s).wait()

        far_done(k - 1)
        far_take(k + 2)

        @pl.when(k > 0)
        def _():
            trail(k - 1)

        far_start(k + 3)

        ready = (c == lax.rem(k + 1, GRID)) & (r == lax.rem(k + 2, GRID)) & (k + 2 < steps)

        @pl.when(ready)
        def _():
            x_stage(k + 1)

        @pl.when(k > 1)
        def _():
            finish(k - 2)

        @pl.when(ready)
        def _():
            @pl.when(k + 1 >= GRID)
            def _():
                pl.semaphore_wait(x_free, 1)
            x_copy(k + 1).start()

        @pl.when((c == lax.rem(k + 1, GRID)) & (k + 1 < steps))
        def _():
            ahead(k)

    @pl.when((r == 1) & (c == 0))
    def _():
        x_stage(0)
        x_copy(0).start()

    loop(0, steps, step)
    far_done(steps - 1)
    finish(steps - 2)
    finish(steps - 1)

    for s in range(nb):
        for t in range(nb):
            store(t, s).wait()


def solution(mesh):
    def factor_local(a_loc):
        nb, blk, width = a_loc.shape
        far = nb * GRID - 1 - far_reach(nb)
        dma = pltpu.SemaphoreType.DMA
        reg = pltpu.SemaphoreType.REGULAR
        work = pl.pallas_call(
            functools.partial(kernel, nb),
            out_shape=jax.ShapeDtypeStruct(a_loc.shape, F32),
            in_specs=[pl.BlockSpec(memory_space=pl.ANY)],
            out_specs=pl.BlockSpec(memory_space=pl.ANY),
            scratch_shapes=[
                pltpu.VMEM((nb, nb * blk, blk), F32),
                pltpu.VMEM((SLOTS, nb * blk, blk), B16),
                pltpu.VMEM((SLOTS, nb * blk, blk), B16),
                pltpu.VMEM((HALF, HALF), F32),
                pltpu.VMEM((HALF, BLK), F32),
                pltpu.VMEM((HALF, HALF), F32),
                pltpu.VMEM((HALF, BLK), F32),
                pltpu.VMEM((BLK, BLK), F32),
                pltpu.VMEM((BLK, BLK), B16),
                pltpu.VMEM((BLK, BLK), F32),
                pltpu.VMEM((hist_at(nb, nb), blk, blk), B16),
                pltpu.VMEM((far, blk, blk), B16),
                dma((nb, nb)),
                dma((SLOTS, nb)),
                dma((SLOTS, nb)),
                dma((GRID - 1, nb)),
                dma((SLOTS, nb)),
                dma((SLOTS, 2, nb)),
                dma((3,)),
                dma((3, 3)),
                dma((3,)),
                dma,
                dma,
                dma,
                dma,
                reg((SLOTS // GRID,)),
                reg((GRID - 1,)),
                reg((2,)),
                reg,
                reg,
                dma((far,)),
                dma((far, 2)),
                reg((2,)),
            ],
            compiler_params=pltpu.CompilerParams(collective_id=0, has_side_effects=True, vmem_limit_bytes=75 * 512 * 1024),
        )(a_loc)
        row_id = lax.axis_index("row")
        col_id = lax.axis_index("col")
        row_blk = jnp.arange(nb) * GRID + row_id
        col_blk = jnp.arange(width // blk) * GRID + col_id
        keep = row_blk[:, None, None, None] >= col_blk[None, None, :, None]
        return jnp.where(keep, work.reshape(nb, blk, width // blk, blk), 0.0).reshape(nb, blk, width)

    spec = P(("batch", "row"), None, "col")
    return jax.shard_map(factor_local, mesh=mesh, in_specs=(spec,), out_specs=spec, check_vma=False)
```

```python
import functools

import jax
import jax.numpy as jnp
from jax import lax
from jax.experimental import pallas as pl
from jax.experimental.pallas import tpu as pltpu
from jax.sharding import PartitionSpec as P

MESH = pl.DeviceIdType.MESH
HIGH = lax.Precision.HIGHEST
GRID = 4
BLK = 256
HALF = 128
PAN = 16
SLOTS = 8
VIA = 1
F32, B16 = jnp.float32, jnp.bfloat16
NT = (((1,), (1,)), ((), ()))
TN = (((0,), (0,)), ((), ()))


def split3(x):
    hi = x.astype(B16)
    rest = x - hi.astype(F32)
    mid = rest.astype(B16)
    return hi, mid, (rest - mid.astype(F32)).astype(B16)


def gram(left, right):
    a1, a2, a3 = split3(left)
    b1, b2, b3 = split3(right)
    lhs = jnp.concatenate([a1, a1, a2, a2, a1, a3], axis=0)
    rhs = jnp.concatenate([b1, b2, b1, b2, b3, b1], axis=0)
    return lax.dot_general(lhs, rhs, TN, preferred_element_type=F32)


def eliminate(rows, base):
    groups = rows.shape[0]
    cols = [jnp.broadcast_to(rows[0][:, base + t : base + t + 1], (PAN, HALF))[None] for t in range(PAN)]
    work = jnp.concatenate(cols + [rows], axis=0)
    sub = lax.broadcasted_iota(jnp.int32, (PAN, HALF), 0)
    scale = jnp.zeros((PAN, HALF), F32)
    for t in range(PAN):
        root = jnp.broadcast_to(lax.rsqrt(work[0, t : t + 1, :]), (PAN, HALF))
        scale = jnp.where(sub == t, root, scale)
        mult = jnp.where(sub > t, work[0] * (root * root), 0.0)
        work = work[1:]
        work = work - mult[None] * work[:, t : t + 1, :]
    return work[-groups:] * scale[None]


def factor_half(tab, emit):
    count = HALF // PAN
    groups = tab.shape[1] // HALF
    done = []
    for p in range(count):
        own = tab[:PAN]
        rows = jnp.concatenate([own[None, :, g * HALF : (g + 1) * HALF] for g in range(groups)], axis=0)
        out = eliminate(rows, p * PAN)
        flat = jnp.concatenate([out[g] for g in range(groups)], axis=1)
        done.append(flat)
        emit(p, flat)
        if p + 1 < count:
            tab = tab[PAN:] - gram(flat[:, :HALF], flat)[(p + 1) * PAN :]
    return jnp.concatenate(done, axis=0)


def far_reach(nb):
    return 21 * nb // 8


def hist_at(t, nb):
    base = (far_reach(nb) + 1) // GRID
    m = t - base
    return m * (GRID * (base + 1) - 1 - far_reach(nb)) + m * (m - 1) * (GRID // 2)


def kernel(nb, a_ref, o_ref, mat, row_pan, col_pan, inv_a, inv_b, nxt_a, nxt_b, nxt_x, nxt_y, x_out, hist, far_col, load_sem, br_recv, bc_recv,
           row_send, relay_send, chain_send, inv_recv, inv_send, nxt_recv, x_recv, x_send, y_recv, y_send, row_free, inv_free, chain_free, nxt_free, x_free, via_free, far_recv, far_send,
           far_free):
    r = lax.axis_index("row")
    c = lax.axis_index("col")
    steps = nb * GRID
    last = GRID * (nb - 1)
    reach = far_reach(nb)
    base = (reach + 1) // GRID

    def first_block(k, pos):
        return lax.div(k + GRID - pos, GRID)

    def rows_of(t):
        return pl.ds(pl.multiple_of(t * BLK, BLK), BLK)

    def load(t, s):
        return pltpu.make_async_copy(a_ref.at[t, :, pl.ds(s * BLK, BLK)], mat.at[s, pl.ds(t * BLK, BLK), :], load_sem.at[t, s])

    def store(t, s):
        return pltpu.make_async_copy(mat.at[s, pl.ds(t * BLK, BLK), :], o_ref.at[t, :, pl.ds(pl.multiple_of(s * BLK, BLK), BLK)], load_sem.at[t, s])

    for s in range(nb):
        for t in range(nb):
            load(t, s).start()

    barrier = pltpu.get_barrier_semaphore()
    for off in range(1, GRID):
        pl.semaphore_signal(barrier, inc=1, device_id={"row": lax.rem(r + off, GRID)}, device_id_type=MESH)
        pl.semaphore_signal(barrier, inc=1, device_id={"col": lax.rem(c + off, GRID)}, device_id_type=MESH)
    for off in (1, GRID - 1):
        pl.semaphore_signal(barrier, inc=1, device_id={"row": lax.rem(r + off, GRID), "col": lax.rem(c + off, GRID)}, device_id_type=MESH)
    pl.semaphore_wait(barrier, 2 * GRID)

    for t in range(nb):
        load(t, 0).wait()

    def row_copy(slot, t, off):
        return pltpu.make_async_remote_copy(
            src_ref=row_pan.at[slot, rows_of(t), :], dst_ref=row_pan.at[slot, rows_of(t), :],
            send_sem=row_send.at[off - 1, t], recv_sem=br_recv.at[slot, t],
            device_id={"col": lax.rem(c + off, GRID)}, device_id_type=MESH)

    def relay_copy(slot, t):
        return pltpu.make_async_remote_copy(
            src_ref=row_pan.at[slot, rows_of(t), :], dst_ref=row_pan.at[slot, rows_of(t), :],
            send_sem=relay_send.at[slot, t], recv_sem=br_recv.at[slot, t],
            device_id={"col": lax.rem(c + 1, GRID)}, device_id_type=MESH)

    def relays(k):
        return (lax.rem(c, 2) == 0) & (lax.div(c, 2) != lax.div(lax.rem(k, GRID), 2))

    def chain_copy(src, slot, s, way):
        return pltpu.make_async_remote_copy(
            src_ref=src.at[slot, rows_of(s), :], dst_ref=col_pan.at[slot, rows_of(s), :],
            send_sem=chain_send.at[slot, way, s], recv_sem=bc_recv.at[slot, s],
            device_id={"row": r + 1 - 2 * way}, device_id_type=MESH)

    def inv_part(a, b, part):
        return a if part == 0 else b.at[pl.ds((part - 1) * (HALF // 2), HALF // 2), :]

    def inv_copy(way, part):
        ref = inv_part(inv_a, inv_b, part)
        return pltpu.make_async_remote_copy(
            src_ref=ref, dst_ref=ref, send_sem=inv_send.at[1 + way, part], recv_sem=inv_recv.at[part],
            device_id={"row": r + 1 - 2 * way}, device_id_type=MESH)

    def inv_ways(k, act):
        for way in range(2):
            @pl.when(sends(way) & (k < last + r + 1 - 2 * way))
            def _():
                act(way)

    def nxt_copy(part):
        return pltpu.make_async_remote_copy(
            src_ref=inv_part(inv_a, inv_b, part), dst_ref=inv_part(nxt_a, nxt_b, part),
            send_sem=inv_send.at[0, part], recv_sem=nxt_recv.at[part],
            device_id={"row": jnp.where(r == VIA, r, lax.rem(r + 1, GRID)), "col": lax.rem(c + 1, GRID)}, device_id_type=MESH)

    def via_copy(part):
        ref = inv_part(nxt_a, nxt_b, part) if part < 3 else nxt_y
        return pltpu.make_async_remote_copy(
            src_ref=ref, dst_ref=ref, send_sem=inv_send.at[0, part] if part < 3 else y_send,
            recv_sem=nxt_recv.at[part] if part < 3 else y_recv,
            device_id={"row": lax.rem(r + 1, GRID)}, device_id_type=MESH)

    def via(k):
        return (lax.rem(k, GRID) == VIA) & (r == VIA) & (c == VIA + 1) & (k + 1 < steps)

    def x_copy(k):
        return pltpu.make_async_remote_copy(
            src_ref=x_out, dst_ref=nxt_x, send_sem=x_send, recv_sem=x_recv,
            device_id={"col": lax.rem(c + 1, GRID)}, device_id_type=MESH)

    def x_stage(k):
        x_out[...] = mat[lax.div(k, GRID), rows_of(lax.div(k + 1, GRID)), :]

    def y_copy(k):
        return pltpu.make_async_remote_copy(
            src_ref=row_pan.at[lax.rem(k, SLOTS), rows_of(lax.div(k + 1, GRID)), :], dst_ref=nxt_y,
            send_sem=y_send, recv_sem=y_recv,
            device_id={"row": jnp.where(r == VIA, r, lax.rem(r + 1, GRID)), "col": lax.rem(c + 1, GRID)}, device_id_type=MESH)

    def gather_inv(a, b):
        return jnp.concatenate([jnp.concatenate([a[...], jnp.zeros((HALF, HALF), F32)], axis=1), b[...]], axis=0)

    def sends(way):
        return ((r >= c) & (r < GRID - 1)) if way == 0 else ((r <= c) & (r > 0))

    def near(k):
        return jnp.minimum(nb, lax.div(k + reach - c, GRID) + 1)

    def pass_on(src, k, s):
        slot = lax.rem(k, SLOTS)
        for way in range(2):
            @pl.when(sends(way) & (s < jnp.minimum(near(k), nb - way)))
            def _():
                @pl.when((s == first_block(k, c)) & (k >= SLOTS))
                def _():
                    pl.semaphore_wait(chain_free.at[way], 1)
                chain_copy(src, slot, s, way).start()

    def own_col_block(k, s):
        slot = lax.rem(k, SLOTS)
        col_pan[slot, rows_of(s), :] = row_pan[slot, rows_of(s), :]
        pass_on(row_pan, k, s)

    def take_row(k, t):
        row_copy(lax.rem(k, SLOTS), t, 1).wait_recv()

        @pl.when(relays(k))
        def _():
            relay_copy(lax.rem(k, SLOTS), t).start()

        @pl.when(r == c)
        def _():
            own_col_block(k, t)

    def take_col(k, s):
        chain_copy(col_pan, lax.rem(k, SLOTS), s, 0).wait_recv()
        pass_on(col_pan, k, s)

    def update(k, t, s, count):
        slot = lax.rem(k, SLOTS)
        span = pl.ds(pl.multiple_of(t * BLK, BLK), count * BLK)
        prod = lax.dot_general(row_pan[slot, span, :], col_pan[slot, rows_of(s), :], NT, preferred_element_type=F32)
        mat[s, span, :] = mat[s, span, :] - prod

    def loop(lo, hi, body):
        def run(i, carry):
            body(i)
            return carry
        lax.fori_loop(lo, hi, run, 0)

    def factor_diag(k):
        t0 = lax.div(k, GRID)
        blk = mat[t0, rows_of(t0), :]
        eye = (lax.broadcasted_iota(jnp.int32, (HALF, HALF), 0) == lax.broadcasted_iota(jnp.int32, (HALF, HALF), 1)).astype(F32)

        def for_peers(act):
            for off in range(1, GRID):
                @pl.when(k < last + lax.rem(r + off, GRID))
                def _():
                    act(off)

        @pl.when(k >= GRID)
        def _():
            for_peers(lambda off: pl.semaphore_wait(inv_free.at[off - 1], 1))

        def send(part):
            @pl.when(k + 1 < steps)
            def _():
                nxt_copy(part).start()
            inv_ways(k, lambda way: inv_copy(way, part).start())

        def emit_top(p, flat):
            inv_a[p * PAN : (p + 1) * PAN, :] = flat[:, 2 * HALF :]
            if p == HALF // PAN - 1:
                send(0)

        def emit_low(p, flat):
            inv_b[p * PAN : (p + 1) * PAN, :] = flat[:, HALF:]
            if (p + 1) % (HALF // PAN // 2) == 0:
                send(2 * (p + 1) // (HALF // PAN))

        top = factor_half(jnp.concatenate([blk[:HALF], eye], axis=1), emit_top)
        mid = lax.dot_general(top[:, HALF : 2 * HALF], top[:, HALF:], TN, precision=HIGH, preferred_element_type=F32)
        low = factor_half(jnp.concatenate([blk[HALF:, HALF:] - mid[:, :HALF], -mid[:, HALF:], eye], axis=1), emit_low)
        zero = jnp.zeros((HALF, HALF), F32)
        up = lax.broadcasted_iota(jnp.int32, (HALF, HALF), 0) <= lax.broadcasted_iota(jnp.int32, (HALF, HALF), 1)
        left = jnp.concatenate([jnp.where(up, top[:, :HALF], 0.0).T, top[:, HALF : 2 * HALF].T], axis=0)
        right = jnp.concatenate([zero, jnp.where(up, low[:, :HALF], 0.0).T], axis=0)
        mat[t0, rows_of(t0), :] = jnp.concatenate([left, right], axis=1)

    def for_row(k, t, act):
        own = (r == lax.rem(k + 1, GRID)) & (t == lax.div(k + 1, GRID))
        odd = lax.rem(c, 2)

        @pl.when(jnp.logical_not(own))
        def _():
            act(1)

        @pl.when(odd == 1)
        def _():
            act(3)

        @pl.when((odd == 0) | own)
        def _():
            act(2)

    def solve_col(k):
        t0 = lax.div(k, GRID)
        slot = lax.rem(k, SLOTS)

        @pl.when(k < last + r)
        def _():
            @pl.when(r != c)
            def _():
                for part in range(3):
                    inv_copy(0, part).wait_recv()
                    inv_ways(k, lambda way: inv_copy(way, part).start())

            @pl.when(k >= SLOTS)
            def _():
                pl.semaphore_wait(row_free.at[lax.rem(lax.div(k, GRID), SLOTS // GRID)], GRID - 1)

        early = (r == lax.rem(k + 1, GRID)) & (k + 1 < steps)

        @pl.when(early)
        def _():
            x_copy(k).wait_send()

        def one(t):
            @pl.when((k > 0) & ((t > first_block(k, r)) | (r == c)))
            def _():
                take_row(k - 1, t)
                update(k - 1, t, t0, 1)
            inv = gather_inv(inv_a, inv_b)
            sol = lax.dot_general(mat[t0, rows_of(t), :], inv, NT, precision=HIGH, preferred_element_type=F32)
            mat[t0, rows_of(t), :] = sol
            row_pan[slot, rows_of(t), :] = sol.astype(B16)
            for_row(k, t, lambda off: row_copy(slot, t, off).start())

            @pl.when(r == c)
            def _():
                own_col_block(k, t)

        loop(first_block(k, r), nb, one)

        @pl.when((k < last + r) | (r == c))
        def _():
            for part in range(3):
                inv_ways(k, lambda way: inv_copy(way, part).wait_send())

        @pl.when((r == c) & (k + 1 < steps))
        def _():
            for part in range(3):
                nxt_copy(part).wait_send()

            @pl.when(k > 0)
            def _():
                y_copy(k - 1).wait_send()

        @pl.when((r != c) & (k + GRID < last + r))
        def _():
            pl.semaphore_signal(inv_free.at[lax.rem(r - c + GRID, GRID) - 1], inc=1, device_id={"row": lax.rem(k, GRID)}, device_id_type=MESH)

    top = nb - jnp.where(r < c, 1, 0)

    def columns(k, lo, hi):
        def column(s):
            first = jnp.maximum(first_block(k, r), s)
            pairs = lax.div(nb - first, 2)
            loop(0, pairs, lambda q: update(k, first + 2 * q, s, 2))

            @pl.when(lax.rem(nb - first, 2) == 1)
            def _():
                update(k, nb - 1, s, 1)

        @pl.when(r != c)
        def _():
            loop(lo, hi, lambda s: take_col(k, s))
        loop(lo, hi, column)

    def trail(k):
        d = lax.rem(k, GRID)
        nxt = lax.rem(k + 1, GRID)
        soon = (c == lax.rem(k + 2, GRID)) & (k + 2 < steps)
        s_lo = first_block(k, c) + jnp.where(c == nxt, 1, 0)

        @pl.when((c != d) & (c != nxt))
        def _():
            loop(first_block(k, r), nb, lambda t: take_row(k, t))

        @pl.when(k < steps - 1 - reach)
        def _():
            for t in range(base, nb):
                @pl.when(k < GRID * t + GRID - 1 - reach)
                def _():
                    hist[hist_at(t, nb) + k] = row_pan[lax.rem(k, SLOTS), t * BLK : (t + 1) * BLK, :]

        hi = jnp.minimum(top, near(k))
        columns(k, s_lo, jnp.where(soon, jnp.minimum(s_lo + 1, hi), hi))

    def far_copy(src, kp, way):
        return pltpu.make_async_remote_copy(
            src_ref=src, dst_ref=far_col.at[kp], send_sem=far_send.at[kp, way], recv_sem=far_recv.at[kp],
            device_id={"row": r + 1 - 2 * way}, device_id_type=MESH)

    def far_sent(j, way):
        return (j > reach) & (j < steps) & (lax.div(j, GRID) < nb - way)

    def far_pass(src, j, kp):
        for way in range(2):
            @pl.when(sends(way) & far_sent(j, way))
            def _():
                @pl.when((kp == 0) & (j - GRID > reach))
                def _():
                    pl.semaphore_wait(far_free.at[way], 1)
                far_copy(src, kp, way).start()

    def far_start(j):
        @pl.when((r == c) & (c == lax.rem(j, GRID)) & (j > reach) & (j < steps))
        def _():
            loop(0, j - reach, lambda kp: far_pass(hist.at[hist_at(lax.div(j, GRID), nb) + kp], j, kp))

    def far_take(j):
        s = lax.div(j, GRID)

        @pl.when((c == lax.rem(j, GRID)) & (j > reach) & (j < steps) & (s < top))
        def _():
            def one(kp):
                @pl.when(r == c)
                def _():
                    far_col[kp] = hist[hist_at(s, nb) + kp]

                @pl.when(r != c)
                def _():
                    far_copy(far_col.at[kp], kp, 0).wait_recv()
                    far_pass(far_col.at[kp], j, kp)

                def tile(t):
                    prod = lax.dot_general(hist[hist_at(t, nb) + kp], far_col[kp], NT, preferred_element_type=F32)
                    mat[s, rows_of(t), :] = mat[s, rows_of(t), :] - prod
                loop(s + jnp.where(r < c, 1, 0), nb, tile)
            loop(0, j - reach, one)

    def far_done(j):
        @pl.when((c == lax.rem(j, GRID)) & (j > reach) & (j < steps))
        def _():
            for way in range(2):
                @pl.when(sends(way) & far_sent(j, way))
                def _():
                    loop(0, j - reach, lambda kp: far_copy(far_col.at[kp], kp, way).wait_send())

                @pl.when(far_sent(j + GRID, way) & ((r > c) if way == 0 else (r < c)))
                def _():
                    pl.semaphore_signal(far_free.at[way], inc=1, device_id={"row": r - 1 + 2 * way}, device_id_type=MESH)

    def finish(k):
        d = lax.rem(k, GRID)

        @pl.when(c == d)
        def _():
            for t in range(nb):
                store(t, lax.div(k, GRID)).start()

            def one(t):
                for_row(k, t, lambda off: row_copy(lax.rem(k, SLOTS), t, off).wait_send())
            loop(first_block(k, r), nb, one)

        @pl.when(relays(k))
        def _():
            made = (r == c) & (c == lax.rem(k + 1, GRID)) & (k + 1 < steps)
            loop(first_block(k, r) + jnp.where(made, 1, 0), nb, lambda t: relay_copy(lax.rem(k, SLOTS), t).wait_send())

        for way in range(2):
            @pl.when(sends(way))
            def _():
                loop(first_block(k, c), jnp.minimum(near(k), nb - way), lambda s: chain_copy(col_pan, lax.rem(k, SLOTS), s, way).wait_send())

        @pl.when((c != d) & (k + SLOTS < last + r))
        def _():
            pl.semaphore_signal(row_free.at[lax.rem(lax.div(k, GRID), SLOTS // GRID)], inc=1, device_id={"col": d}, device_id_type=MESH)

        for way in range(2):
            @pl.when((k + SLOTS < last - way * GRID + c) & ((r > c) if way == 0 else (r < c)))
            def _():
                pl.semaphore_signal(chain_free.at[way], inc=1, device_id={"row": r - 1 + 2 * way}, device_id_type=MESH)

    def ahead(k):
        s1 = lax.div(k + 1, GRID)

        @pl.when(r == c)
        def _():
            slot = lax.rem(k, SLOTS)
            x_copy(k).wait_recv()

            @pl.when(k > 0)
            def _():
                y_copy(k - 1).wait_recv()
                prod = lax.dot_general(row_pan[lax.rem(k - 1 + SLOTS, SLOTS), rows_of(s1), :], nxt_y[...], NT, preferred_element_type=F32)
                nxt_x[...] = nxt_x[...] - prod
            for part in range(3):
                nxt_copy(part).wait_recv()
            sol = lax.dot_general(nxt_x[...], gather_inv(nxt_a, nxt_b), NT, precision=HIGH, preferred_element_type=F32).astype(B16)
            row_pan[slot, rows_of(s1), :] = sol
            col_pan[slot, rows_of(s1), :] = sol
            mat[s1, rows_of(s1), :] = mat[s1, rows_of(s1), :] - lax.dot_general(sol, sol, NT, preferred_element_type=F32)

            @pl.when(k + 2 < steps)
            def _():
                @pl.when(k + 1 >= GRID)
                def _():
                    pl.semaphore_wait(nxt_free, 1)

                @pl.when((k + 1 >= GRID + VIA) & (r == VIA))
                def _():
                    pl.semaphore_wait(via_free, 1)
                y_copy(k).start()
            pass_on(row_pan, k, s1)

            @pl.when(k + GRID + 1 < steps)
            def _():
                pl.semaphore_signal(x_free, inc=1, device_id={"col": lax.rem(k, GRID)}, device_id_type=MESH)
                pl.semaphore_signal(nxt_free, inc=1, device_id={"row": lax.rem(k, GRID), "col": lax.rem(k, GRID)}, device_id_type=MESH)

        @pl.when(r != c)
        def _():
            @pl.when(s1 < top)
            def _():
                take_col(k, s1)

            t = first_block(k, r)

            @pl.when(t < nb)
            def _():
                take_row(k, t)
                update(k, t, s1, 1)

    def step(k):
        d = lax.rem(k, GRID)

        @pl.when(c == d)
        def _():
            @pl.when(r == d)
            def _():
                factor_diag(k)
            solve_col(k)

            @pl.when(k > 1)
            def _():
                columns(k - 2, lax.div(k, GRID) + 1, jnp.minimum(top, near(k - 2)))

        @pl.when(k == 1)
        def _():
            for s in range(1, nb):
                for t in range(nb):
                    load(t, s).wait()

        @pl.when(via(k))
        def _():
            for part in (3, 0, 1, 2):
                via_copy(part).wait_recv()
                via_copy(part).start()

        far_done(k - 1)
        far_take(k + 2)

        @pl.when(k > 0)
        def _():
            trail(k - 1)

        far_start(k + 3)

        ready = (c == lax.rem(k + 1, GRID)) & (r == lax.rem(k + 2, GRID)) & (k + 2 < steps)

        @pl.when(ready)
        def _():
            x_stage(k + 1)

        @pl.when(k > 1)
        def _():
            finish(k - 2)

        @pl.when(ready)
        def _():
            @pl.when(k + 1 >= GRID)
            def _():
                pl.semaphore_wait(x_free, 1)
            x_copy(k + 1).start()

        @pl.when((c == lax.rem(k + 1, GRID)) & (k + 1 < steps))
        def _():
            ahead(k)

        @pl.when(via(k))
        def _():
            for part in range(4):
                via_copy(part).wait_send()

            @pl.when(k + GRID + 1 < steps)
            def _():
                pl.semaphore_signal(via_free, inc=1, device_id={"col": VIA}, device_id_type=MESH)

    @pl.when((r == 1) & (c == 0))
    def _():
        x_stage(0)
        x_copy(0).start()

    loop(0, steps, step)
    far_done(steps - 1)
    finish(steps - 2)
    finish(steps - 1)

    for s in range(nb):
        for t in range(nb):
            store(t, s).wait()


def solution(mesh):
    def factor_local(a_loc):
        nb, blk, width = a_loc.shape
        far = nb * GRID - 1 - far_reach(nb)
        dma = pltpu.SemaphoreType.DMA
        reg = pltpu.SemaphoreType.REGULAR
        work = pl.pallas_call(
            functools.partial(kernel, nb),
            out_shape=jax.ShapeDtypeStruct(a_loc.shape, F32),
            in_specs=[pl.BlockSpec(memory_space=pl.ANY)],
            out_specs=pl.BlockSpec(memory_space=pl.ANY),
            scratch_shapes=[
                pltpu.VMEM((nb, nb * blk, blk), F32),
                pltpu.VMEM((SLOTS, nb * blk, blk), B16),
                pltpu.VMEM((SLOTS, nb * blk, blk), B16),
                pltpu.VMEM((HALF, HALF), F32),
                pltpu.VMEM((HALF, BLK), F32),
                pltpu.VMEM((HALF, HALF), F32),
                pltpu.VMEM((HALF, BLK), F32),
                pltpu.VMEM((BLK, BLK), F32),
                pltpu.VMEM((BLK, BLK), B16),
                pltpu.VMEM((BLK, BLK), F32),
                pltpu.VMEM((hist_at(nb, nb), blk, blk), B16),
                pltpu.VMEM((far, blk, blk), B16),
                dma((nb, nb)),
                dma((SLOTS, nb)),
                dma((SLOTS, nb)),
                dma((GRID - 1, nb)),
                dma((SLOTS, nb)),
                dma((SLOTS, 2, nb)),
                dma((3,)),
                dma((3, 3)),
                dma((3,)),
                dma,
                dma,
                dma,
                dma,
                reg((SLOTS // GRID,)),
                reg((GRID - 1,)),
                reg((2,)),
                reg,
                reg,
                reg,
                dma((far,)),
                dma((far, 2)),
                reg((2,)),
            ],
            compiler_params=pltpu.CompilerParams(collective_id=0, has_side_effects=True, vmem_limit_bytes=75 * 512 * 1024),
        )(a_loc)
        row_id = lax.axis_index("row")
        col_id = lax.axis_index("col")
        row_blk = jnp.arange(nb) * GRID + row_id
        col_blk = jnp.arange(width // blk) * GRID + col_id
        keep = row_blk[:, None, None, None] >= col_blk[None, None, :, None]
        return jnp.where(keep, work.reshape(nb, blk, width // blk, blk), 0.0).reshape(nb, blk, width)

    spec = P(("batch", "row"), None, "col")
    return jax.shard_map(factor_local, mesh=mesh, in_specs=(spec,), out_specs=spec, check_vma=False)
```

```python
import functools

import jax
import jax.numpy as jnp
from jax import lax
from jax.experimental import pallas as pl
from jax.experimental.pallas import tpu as pltpu
from jax.sharding import PartitionSpec as P

MESH = pl.DeviceIdType.MESH
HIGH = lax.Precision.HIGHEST
GRID = 4
BLK = 256
HALF = 128
PAN = 16
SLOTS = 8
VIA = 1
F32, B16 = jnp.float32, jnp.bfloat16
NT = (((1,), (1,)), ((), ()))
TN = (((0,), (0,)), ((), ()))


def split3(x):
    hi = x.astype(B16)
    rest = x - hi.astype(F32)
    mid = rest.astype(B16)
    return hi, mid, (rest - mid.astype(F32)).astype(B16)


def gram(left, right):
    a1, a2, a3 = split3(left)
    b1, b2, b3 = split3(right)
    lhs = jnp.concatenate([a1, a1, a2, a2, a1, a3], axis=0)
    rhs = jnp.concatenate([b1, b2, b1, b2, b3, b1], axis=0)
    return lax.dot_general(lhs, rhs, TN, preferred_element_type=F32)


def eliminate(rows, base):
    groups = rows.shape[0]
    cols = [jnp.broadcast_to(rows[0][:, base + t : base + t + 1], (PAN, HALF))[None] for t in range(PAN)]
    work = jnp.concatenate(cols + [rows], axis=0)
    sub = lax.broadcasted_iota(jnp.int32, (PAN, HALF), 0)
    scale = jnp.zeros((PAN, HALF), F32)
    for t in range(PAN):
        root = jnp.broadcast_to(lax.rsqrt(work[0, t : t + 1, :]), (PAN, HALF))
        scale = jnp.where(sub == t, root, scale)
        mult = jnp.where(sub > t, work[0] * (root * root), 0.0)
        work = work[1:]
        work = work - mult[None] * work[:, t : t + 1, :]
    return work[-groups:] * scale[None]


def factor_half(tab, emit):
    count = HALF // PAN
    groups = tab.shape[1] // HALF
    done = []
    for p in range(count):
        own = tab[:PAN]
        rows = jnp.concatenate([own[None, :, g * HALF : (g + 1) * HALF] for g in range(groups)], axis=0)
        out = eliminate(rows, p * PAN)
        flat = jnp.concatenate([out[g] for g in range(groups)], axis=1)
        done.append(flat)
        emit(p, flat)
        if p + 1 < count:
            tab = tab[PAN:] - gram(flat[:, :HALF], flat)[(p + 1) * PAN :]
    return jnp.concatenate(done, axis=0)


def far_reach(nb):
    return 21 * nb // 8


def hist_at(t, nb):
    base = (far_reach(nb) + 1) // GRID
    m = t - base
    return m * (GRID * (base + 1) - 1 - far_reach(nb)) + m * (m - 1) * (GRID // 2)


def kernel(nb, a_ref, o_ref, mat, row_pan, col_pan, inv_a, inv_b, nxt_a, nxt_b, nxt_x, nxt_y, x_out, hist, far_col, load_sem, br_recv, bc_recv,
           row_send, relay_send, chain_send, inv_recv, inv_send, nxt_recv, x_recv, x_send, y_recv, y_send, row_free, inv_free, chain_free, nxt_free, x_free, via_free, far_recv, far_send,
           far_free):
    r = lax.axis_index("row")
    c = lax.axis_index("col")
    steps = nb * GRID
    last = GRID * (nb - 1)
    reach = far_reach(nb)
    base = (reach + 1) // GRID

    def first_block(k, pos):
        return lax.div(k + GRID - pos, GRID)

    def rows_of(t):
        return pl.ds(pl.multiple_of(t * BLK, BLK), BLK)

    def load(t, s):
        return pltpu.make_async_copy(a_ref.at[t, :, pl.ds(s * BLK, BLK)], mat.at[s, pl.ds(t * BLK, BLK), :], load_sem.at[t, s])

    def store(t, s):
        return pltpu.make_async_copy(mat.at[s, pl.ds(t * BLK, BLK), :], o_ref.at[t, :, pl.ds(pl.multiple_of(s * BLK, BLK), BLK)], load_sem.at[t, s])

    for s in range(nb):
        for t in range(nb):
            load(t, s).start()

    barrier = pltpu.get_barrier_semaphore()
    for off in range(1, GRID):
        pl.semaphore_signal(barrier, inc=1, device_id={"row": lax.rem(r + off, GRID)}, device_id_type=MESH)
        pl.semaphore_signal(barrier, inc=1, device_id={"col": lax.rem(c + off, GRID)}, device_id_type=MESH)
    for off in (1, GRID - 1):
        pl.semaphore_signal(barrier, inc=1, device_id={"row": lax.rem(r + off, GRID), "col": lax.rem(c + off, GRID)}, device_id_type=MESH)
    pl.semaphore_wait(barrier, 2 * GRID)

    for t in range(nb):
        load(t, 0).wait()

    def row_copy(slot, t, off):
        return pltpu.make_async_remote_copy(
            src_ref=row_pan.at[slot, rows_of(t), :], dst_ref=row_pan.at[slot, rows_of(t), :],
            send_sem=row_send.at[off - 1, t], recv_sem=br_recv.at[slot, t],
            device_id={"col": lax.rem(c + off, GRID)}, device_id_type=MESH)

    def relay_copy(slot, t):
        return pltpu.make_async_remote_copy(
            src_ref=row_pan.at[slot, rows_of(t), :], dst_ref=row_pan.at[slot, rows_of(t), :],
            send_sem=relay_send.at[slot, t], recv_sem=br_recv.at[slot, t],
            device_id={"col": lax.rem(c + 1, GRID)}, device_id_type=MESH)

    def relays(k):
        return (lax.rem(c, 2) == 0) & (lax.div(c, 2) != lax.div(lax.rem(k, GRID), 2))

    def chain_copy(src, slot, s, way):
        return pltpu.make_async_remote_copy(
            src_ref=src.at[slot, rows_of(s), :], dst_ref=col_pan.at[slot, rows_of(s), :],
            send_sem=chain_send.at[slot, way, s], recv_sem=bc_recv.at[slot, s],
            device_id={"row": r + 1 - 2 * way}, device_id_type=MESH)

    def inv_part(a, b, part):
        return a if part == 0 else b.at[pl.ds((part - 1) * (HALF // 2), HALF // 2), :]

    def inv_copy(way, part):
        ref = inv_part(inv_a, inv_b, part)
        return pltpu.make_async_remote_copy(
            src_ref=ref, dst_ref=ref, send_sem=inv_send.at[1 + way, part], recv_sem=inv_recv.at[part],
            device_id={"row": r + 1 - 2 * way}, device_id_type=MESH)

    def inv_ways(k, act):
        for way in range(2):
            @pl.when(sends(way) & (k < last + r + 1 - 2 * way))
            def _():
                act(way)

    def nxt_copy(part):
        return pltpu.make_async_remote_copy(
            src_ref=inv_part(inv_a, inv_b, part), dst_ref=inv_part(nxt_a, nxt_b, part),
            send_sem=inv_send.at[0, part], recv_sem=nxt_recv.at[part],
            device_id={"row": jnp.where(r == VIA, r, lax.rem(r + 1, GRID)), "col": lax.rem(c + 1, GRID)}, device_id_type=MESH)

    def hand_copy(part):
        return pltpu.make_async_remote_copy(
            src_ref=inv_part(inv_a, inv_b, part), dst_ref=inv_part(nxt_a, nxt_b, part),
            send_sem=inv_send.at[0, part], recv_sem=nxt_recv.at[part],
            device_id={"col": lax.rem(c + 1, GRID)}, device_id_type=MESH)

    def hands(k):
        return (lax.rem(k, 2) == 0) & (r == lax.rem(k + 1, GRID))

    def via_copy(part):
        ref = inv_part(nxt_a, nxt_b, part) if part < 3 else nxt_y
        return pltpu.make_async_remote_copy(
            src_ref=ref, dst_ref=ref, send_sem=inv_send.at[0, part] if part < 3 else y_send,
            recv_sem=nxt_recv.at[part] if part < 3 else y_recv,
            device_id={"row": lax.rem(r + 1, GRID)}, device_id_type=MESH)

    def via(k):
        return (lax.rem(k, GRID) == VIA) & (r == VIA) & (c == VIA + 1) & (k + 1 < steps)

    def x_copy(k):
        return pltpu.make_async_remote_copy(
            src_ref=x_out, dst_ref=nxt_x, send_sem=x_send, recv_sem=x_recv,
            device_id={"col": lax.rem(c + 1, GRID)}, device_id_type=MESH)

    def x_stage(k):
        x_out[...] = mat[lax.div(k, GRID), rows_of(lax.div(k + 1, GRID)), :]

    def y_copy(k):
        return pltpu.make_async_remote_copy(
            src_ref=row_pan.at[lax.rem(k, SLOTS), rows_of(lax.div(k + 1, GRID)), :], dst_ref=nxt_y,
            send_sem=y_send, recv_sem=y_recv,
            device_id={"row": jnp.where(r == VIA, r, lax.rem(r + 1, GRID)), "col": lax.rem(c + 1, GRID)}, device_id_type=MESH)

    def gather_inv(a, b):
        return jnp.concatenate([jnp.concatenate([a[...], jnp.zeros((HALF, HALF), F32)], axis=1), b[...]], axis=0)

    def sends(way):
        return ((r >= c) & (r < GRID - 1)) if way == 0 else ((r <= c) & (r > 0))

    def near(k):
        return jnp.minimum(nb, lax.div(k + reach - c, GRID) + 1)

    def pass_on(src, k, s):
        slot = lax.rem(k, SLOTS)
        for way in range(2):
            @pl.when(sends(way) & (s < jnp.minimum(near(k), nb - way)))
            def _():
                @pl.when((s == first_block(k, c)) & (k >= SLOTS))
                def _():
                    pl.semaphore_wait(chain_free.at[way], 1)
                chain_copy(src, slot, s, way).start()

    def own_col_block(k, s):
        slot = lax.rem(k, SLOTS)
        col_pan[slot, rows_of(s), :] = row_pan[slot, rows_of(s), :]
        pass_on(row_pan, k, s)

    def take_row(k, t):
        row_copy(lax.rem(k, SLOTS), t, 1).wait_recv()

        @pl.when(relays(k))
        def _():
            relay_copy(lax.rem(k, SLOTS), t).start()

        @pl.when(r == c)
        def _():
            own_col_block(k, t)

    def take_col(k, s):
        chain_copy(col_pan, lax.rem(k, SLOTS), s, 0).wait_recv()
        pass_on(col_pan, k, s)

    def update(k, t, s, count):
        slot = lax.rem(k, SLOTS)
        span = pl.ds(pl.multiple_of(t * BLK, BLK), count * BLK)
        prod = lax.dot_general(row_pan[slot, span, :], col_pan[slot, rows_of(s), :], NT, preferred_element_type=F32)
        mat[s, span, :] = mat[s, span, :] - prod

    def loop(lo, hi, body):
        def run(i, carry):
            body(i)
            return carry
        lax.fori_loop(lo, hi, run, 0)

    def factor_diag(k):
        t0 = lax.div(k, GRID)
        blk = mat[t0, rows_of(t0), :]
        eye = (lax.broadcasted_iota(jnp.int32, (HALF, HALF), 0) == lax.broadcasted_iota(jnp.int32, (HALF, HALF), 1)).astype(F32)

        def for_peers(act):
            for off in range(1, GRID):
                @pl.when(k < last + lax.rem(r + off, GRID))
                def _():
                    act(off)

        @pl.when(k >= GRID)
        def _():
            for_peers(lambda off: pl.semaphore_wait(inv_free.at[off - 1], 1))

        def send(part):
            @pl.when((k + 1 < steps) & (lax.rem(k, 2) == 1))
            def _():
                nxt_copy(part).start()
            inv_ways(k, lambda way: inv_copy(way, part).start())

        def emit_top(p, flat):
            inv_a[p * PAN : (p + 1) * PAN, :] = flat[:, 2 * HALF :]
            if p == HALF // PAN - 1:
                send(0)

        def emit_low(p, flat):
            inv_b[p * PAN : (p + 1) * PAN, :] = flat[:, HALF:]
            if (p + 1) % (HALF // PAN // 2) == 0:
                send(2 * (p + 1) // (HALF // PAN))

        top = factor_half(jnp.concatenate([blk[:HALF], eye], axis=1), emit_top)
        mid = lax.dot_general(top[:, HALF : 2 * HALF], top[:, HALF:], TN, precision=HIGH, preferred_element_type=F32)
        low = factor_half(jnp.concatenate([blk[HALF:, HALF:] - mid[:, :HALF], -mid[:, HALF:], eye], axis=1), emit_low)
        zero = jnp.zeros((HALF, HALF), F32)
        up = lax.broadcasted_iota(jnp.int32, (HALF, HALF), 0) <= lax.broadcasted_iota(jnp.int32, (HALF, HALF), 1)
        left = jnp.concatenate([jnp.where(up, top[:, :HALF], 0.0).T, top[:, HALF : 2 * HALF].T], axis=0)
        right = jnp.concatenate([zero, jnp.where(up, low[:, :HALF], 0.0).T], axis=0)
        mat[t0, rows_of(t0), :] = jnp.concatenate([left, right], axis=1)

    def for_row(k, t, act):
        own = (r == lax.rem(k + 1, GRID)) & (t == lax.div(k + 1, GRID))
        odd = lax.rem(c, 2)

        @pl.when(jnp.logical_not(own))
        def _():
            act(1)

        @pl.when(odd == 1)
        def _():
            act(3)

        @pl.when((odd == 0) | own)
        def _():
            act(2)

    def solve_col(k):
        t0 = lax.div(k, GRID)
        slot = lax.rem(k, SLOTS)

        @pl.when(k < last + r)
        def _():
            @pl.when(r != c)
            def _():
                for part in range(3):
                    inv_copy(0, part).wait_recv()

                    @pl.when(hands(k))
                    def _():
                        hand_copy(part).start()
                    inv_ways(k, lambda way: inv_copy(way, part).start())

            @pl.when(k >= SLOTS)
            def _():
                pl.semaphore_wait(row_free.at[lax.rem(lax.div(k, GRID), SLOTS // GRID)], GRID - 1)

        early = (r == lax.rem(k + 1, GRID)) & (k + 1 < steps)

        @pl.when(early)
        def _():
            x_copy(k).wait_send()

        def one(t):
            @pl.when((k > 0) & ((t > first_block(k, r)) | (r == c)))
            def _():
                take_row(k - 1, t)
                update(k - 1, t, t0, 1)
            inv = gather_inv(inv_a, inv_b)
            sol = lax.dot_general(mat[t0, rows_of(t), :], inv, NT, precision=HIGH, preferred_element_type=F32)
            mat[t0, rows_of(t), :] = sol
            row_pan[slot, rows_of(t), :] = sol.astype(B16)
            for_row(k, t, lambda off: row_copy(slot, t, off).start())

            @pl.when(r == c)
            def _():
                own_col_block(k, t)

        loop(first_block(k, r), nb, one)

        @pl.when((k < last + r) | (r == c))
        def _():
            for part in range(3):
                inv_ways(k, lambda way: inv_copy(way, part).wait_send())

        @pl.when((k < last + r) & hands(k))
        def _():
            for part in range(3):
                hand_copy(part).wait_send()

        @pl.when((r == c) & (k + 1 < steps))
        def _():
            @pl.when(lax.rem(k, 2) == 1)
            def _():
                for part in range(3):
                    nxt_copy(part).wait_send()

            @pl.when(k > 0)
            def _():
                y_copy(k - 1).wait_send()

        @pl.when((r != c) & (k + GRID < last + r))
        def _():
            pl.semaphore_signal(inv_free.at[lax.rem(r - c + GRID, GRID) - 1], inc=1, device_id={"row": lax.rem(k, GRID)}, device_id_type=MESH)

    top = nb - jnp.where(r < c, 1, 0)

    def columns(k, lo, hi):
        def column(s):
            first = jnp.maximum(first_block(k, r), s)
            pairs = lax.div(nb - first, 2)
            loop(0, pairs, lambda q: update(k, first + 2 * q, s, 2))

            @pl.when(lax.rem(nb - first, 2) == 1)
            def _():
                update(k, nb - 1, s, 1)

        @pl.when(r != c)
        def _():
            loop(lo, hi, lambda s: take_col(k, s))
        loop(lo, hi, column)

    def trail(k):
        d = lax.rem(k, GRID)
        nxt = lax.rem(k + 1, GRID)
        soon = (c == lax.rem(k + 2, GRID)) & (k + 2 < steps)
        s_lo = first_block(k, c) + jnp.where(c == nxt, 1, 0)

        @pl.when((c != d) & (c != nxt))
        def _():
            loop(first_block(k, r), nb, lambda t: take_row(k, t))

        @pl.when(k < steps - 1 - reach)
        def _():
            for t in range(base, nb):
                @pl.when(k < GRID * t + GRID - 1 - reach)
                def _():
                    hist[hist_at(t, nb) + k] = row_pan[lax.rem(k, SLOTS), t * BLK : (t + 1) * BLK, :]

        hi = jnp.minimum(top, near(k))
        columns(k, s_lo, jnp.where(soon, jnp.minimum(s_lo + 1, hi), hi))

    def far_copy(src, kp, way):
        return pltpu.make_async_remote_copy(
            src_ref=src, dst_ref=far_col.at[kp], send_sem=far_send.at[kp, way], recv_sem=far_recv.at[kp],
            device_id={"row": r + 1 - 2 * way}, device_id_type=MESH)

    def far_sent(j, way):
        return (j > reach) & (j < steps) & (lax.div(j, GRID) < nb - way)

    def far_pass(src, j, kp):
        for way in range(2):
            @pl.when(sends(way) & far_sent(j, way))
            def _():
                @pl.when((kp == 0) & (j - GRID > reach))
                def _():
                    pl.semaphore_wait(far_free.at[way], 1)
                far_copy(src, kp, way).start()

    def far_start(j):
        @pl.when((r == c) & (c == lax.rem(j, GRID)) & (j > reach) & (j < steps))
        def _():
            loop(0, j - reach, lambda kp: far_pass(hist.at[hist_at(lax.div(j, GRID), nb) + kp], j, kp))

    def far_take(j):
        s = lax.div(j, GRID)

        @pl.when((c == lax.rem(j, GRID)) & (j > reach) & (j < steps) & (s < top))
        def _():
            def one(kp):
                @pl.when(r == c)
                def _():
                    far_col[kp] = hist[hist_at(s, nb) + kp]

                @pl.when(r != c)
                def _():
                    far_copy(far_col.at[kp], kp, 0).wait_recv()
                    far_pass(far_col.at[kp], j, kp)

                def tile(t):
                    prod = lax.dot_general(hist[hist_at(t, nb) + kp], far_col[kp], NT, preferred_element_type=F32)
                    mat[s, rows_of(t), :] = mat[s, rows_of(t), :] - prod
                loop(s + jnp.where(r < c, 1, 0), nb, tile)
            loop(0, j - reach, one)

    def far_done(j):
        @pl.when((c == lax.rem(j, GRID)) & (j > reach) & (j < steps))
        def _():
            for way in range(2):
                @pl.when(sends(way) & far_sent(j, way))
                def _():
                    loop(0, j - reach, lambda kp: far_copy(far_col.at[kp], kp, way).wait_send())

                @pl.when(far_sent(j + GRID, way) & ((r > c) if way == 0 else (r < c)))
                def _():
                    pl.semaphore_signal(far_free.at[way], inc=1, device_id={"row": r - 1 + 2 * way}, device_id_type=MESH)

    def finish(k):
        d = lax.rem(k, GRID)

        @pl.when(c == d)
        def _():
            for t in range(nb):
                store(t, lax.div(k, GRID)).start()

            def one(t):
                for_row(k, t, lambda off: row_copy(lax.rem(k, SLOTS), t, off).wait_send())
            loop(first_block(k, r), nb, one)

        @pl.when(relays(k))
        def _():
            made = (r == c) & (c == lax.rem(k + 1, GRID)) & (k + 1 < steps)
            loop(first_block(k, r) + jnp.where(made, 1, 0), nb, lambda t: relay_copy(lax.rem(k, SLOTS), t).wait_send())

        for way in range(2):
            @pl.when(sends(way))
            def _():
                loop(first_block(k, c), jnp.minimum(near(k), nb - way), lambda s: chain_copy(col_pan, lax.rem(k, SLOTS), s, way).wait_send())

        @pl.when((c != d) & (k + SLOTS < last + r))
        def _():
            pl.semaphore_signal(row_free.at[lax.rem(lax.div(k, GRID), SLOTS // GRID)], inc=1, device_id={"col": d}, device_id_type=MESH)

        for way in range(2):
            @pl.when((k + SLOTS < last - way * GRID + c) & ((r > c) if way == 0 else (r < c)))
            def _():
                pl.semaphore_signal(chain_free.at[way], inc=1, device_id={"row": r - 1 + 2 * way}, device_id_type=MESH)

    def ahead(k):
        s1 = lax.div(k + 1, GRID)

        @pl.when(r == c)
        def _():
            slot = lax.rem(k, SLOTS)
            x_copy(k).wait_recv()

            @pl.when(k > 0)
            def _():
                y_copy(k - 1).wait_recv()
                prod = lax.dot_general(row_pan[lax.rem(k - 1 + SLOTS, SLOTS), rows_of(s1), :], nxt_y[...], NT, preferred_element_type=F32)
                nxt_x[...] = nxt_x[...] - prod
            for part in range(3):
                nxt_copy(part).wait_recv()
            sol = lax.dot_general(nxt_x[...], gather_inv(nxt_a, nxt_b), NT, precision=HIGH, preferred_element_type=F32).astype(B16)
            row_pan[slot, rows_of(s1), :] = sol
            col_pan[slot, rows_of(s1), :] = sol
            mat[s1, rows_of(s1), :] = mat[s1, rows_of(s1), :] - lax.dot_general(sol, sol, NT, preferred_element_type=F32)

            @pl.when(k + 2 < steps)
            def _():
                @pl.when(k + 1 >= GRID)
                def _():
                    pl.semaphore_wait(nxt_free, 1)

                @pl.when((k + 1 >= GRID + VIA) & (r == VIA))
                def _():
                    pl.semaphore_wait(via_free, 1)
                y_copy(k).start()
            pass_on(row_pan, k, s1)

            @pl.when(k + GRID + 1 < steps)
            def _():
                pl.semaphore_signal(x_free, inc=1, device_id={"col": lax.rem(k, GRID)}, device_id_type=MESH)
                pl.semaphore_signal(nxt_free, inc=1, device_id={"row": lax.rem(k, GRID), "col": lax.rem(k, GRID)}, device_id_type=MESH)

        @pl.when(r != c)
        def _():
            @pl.when(s1 < top)
            def _():
                take_col(k, s1)

            t = first_block(k, r)

            @pl.when(t < nb)
            def _():
                take_row(k, t)
                update(k, t, s1, 1)

    def step(k):
        d = lax.rem(k, GRID)

        @pl.when(c == d)
        def _():
            @pl.when(r == d)
            def _():
                factor_diag(k)
            solve_col(k)

            @pl.when(k > 1)
            def _():
                columns(k - 2, lax.div(k, GRID) + 1, jnp.minimum(top, near(k - 2)))

        @pl.when(k == 1)
        def _():
            for s in range(1, nb):
                for t in range(nb):
                    load(t, s).wait()

        @pl.when(via(k))
        def _():
            for part in (3, 0, 1, 2):
                via_copy(part).wait_recv()
                via_copy(part).start()

        far_done(k - 1)
        far_take(k + 2)

        @pl.when(k > 0)
        def _():
            trail(k - 1)

        far_start(k + 3)

        ready = (c == lax.rem(k + 1, GRID)) & (r == lax.rem(k + 2, GRID)) & (k + 2 < steps)

        @pl.when(ready)
        def _():
            x_stage(k + 1)

        @pl.when(k > 1)
        def _():
            finish(k - 2)

        @pl.when(ready)
        def _():
            @pl.when(k + 1 >= GRID)
            def _():
                pl.semaphore_wait(x_free, 1)
            x_copy(k + 1).start()

        @pl.when((c == lax.rem(k + 1, GRID)) & (k + 1 < steps))
        def _():
            ahead(k)

        @pl.when(via(k))
        def _():
            for part in range(4):
                via_copy(part).wait_send()

            @pl.when(k + GRID + 1 < steps)
            def _():
                pl.semaphore_signal(via_free, inc=1, device_id={"col": VIA}, device_id_type=MESH)

    @pl.when((r == 1) & (c == 0))
    def _():
        x_stage(0)
        x_copy(0).start()

    loop(0, steps, step)
    far_done(steps - 1)
    finish(steps - 2)
    finish(steps - 1)

    for s in range(nb):
        for t in range(nb):
            store(t, s).wait()


def solution(mesh):
    def factor_local(a_loc):
        nb, blk, width = a_loc.shape
        far = nb * GRID - 1 - far_reach(nb)
        dma = pltpu.SemaphoreType.DMA
        reg = pltpu.SemaphoreType.REGULAR
        work = pl.pallas_call(
            functools.partial(kernel, nb),
            out_shape=jax.ShapeDtypeStruct(a_loc.shape, F32),
            in_specs=[pl.BlockSpec(memory_space=pl.ANY)],
            out_specs=pl.BlockSpec(memory_space=pl.ANY),
            scratch_shapes=[
                pltpu.VMEM((nb, nb * blk, blk), F32),
                pltpu.VMEM((SLOTS, nb * blk, blk), B16),
                pltpu.VMEM((SLOTS, nb * blk, blk), B16),
                pltpu.VMEM((HALF, HALF), F32),
                pltpu.VMEM((HALF, BLK), F32),
                pltpu.VMEM((HALF, HALF), F32),
                pltpu.VMEM((HALF, BLK), F32),
                pltpu.VMEM((BLK, BLK), F32),
                pltpu.VMEM((BLK, BLK), B16),
                pltpu.VMEM((BLK, BLK), F32),
                pltpu.VMEM((hist_at(nb, nb), blk, blk), B16),
                pltpu.VMEM((far, blk, blk), B16),
                dma((nb, nb)),
                dma((SLOTS, nb)),
                dma((SLOTS, nb)),
                dma((GRID - 1, nb)),
                dma((SLOTS, nb)),
                dma((SLOTS, 2, nb)),
                dma((3,)),
                dma((3, 3)),
                dma((3,)),
                dma,
                dma,
                dma,
                dma,
                reg((SLOTS // GRID,)),
                reg((GRID - 1,)),
                reg((2,)),
                reg,
                reg,
                reg,
                dma((far,)),
                dma((far, 2)),
                reg((2,)),
            ],
            compiler_params=pltpu.CompilerParams(collective_id=0, has_side_effects=True, vmem_limit_bytes=75 * 512 * 1024),
        )(a_loc)
        row_id = lax.axis_index("row")
        col_id = lax.axis_index("col")
        row_blk = jnp.arange(nb) * GRID + row_id
        col_blk = jnp.arange(width // blk) * GRID + col_id
        keep = row_blk[:, None, None, None] >= col_blk[None, None, :, None]
        return jnp.where(keep, work.reshape(nb, blk, width // blk, blk), 0.0).reshape(nb, blk, width)

    spec = P(("batch", "row"), None, "col")
    return jax.shard_map(factor_local, mesh=mesh, in_specs=(spec,), out_specs=spec, check_vma=False)
```
